32 devices in a mesh: ta: 8 (over y, x, core), gz: 4 (over z).
Axes of the slice: x: 2, y: 2, z: 4, core: 2. Of those that a mesh axis runs over, the one named last changes fastest.
Arguments:
- source: bfloat16 [8, 4, 2, 4, 3, 12, 256], P('ta', 'gz'), may hold values from -6 to 6
- gauge_field: bfloat16 [8, 4, 4, 2, 3, 3, 256], P('ta', 'gz'), may hold values from -2.5 to 2.5
Outputs:
- twice_applied: bfloat16 [8, 4, 2, 4, 3, 12, 256], P('ta', 'gz')
The draws below stay inside these ranges and needn't reach their ends.
All inputs are finite; a program needn't handle non-finite values.
Results may differ from the reference program's by a relative error of at most 0.0075.
Values may be sent and summed in bfloat16 or wider, within the bound.
A program may use at most 64 MiB of HBM per device.

```python
import jax
import jax.numpy as jnp
from jax import lax

SPINS = 4
COLORS = 3
RHS = 12
NY = 16
NX = 16
NT = 8
NZ = 4
SITES = 256


def steps_of(stream_key, extent, pieces, least, largest):
    factor_of, own = 1.0, jax.random.fold_in(stream_key, 6)
    for axis_at, parts in pieces:
        steps = jnp.exp(jax.random.uniform(jax.random.fold_in(own, axis_at), (parts,), jnp.float32, least / len(pieces), largest / len(pieces)))
        factor_of = factor_of * jnp.repeat(steps, extent[axis_at] // parts).reshape([-1 if axis == axis_at else 1 for axis in range(len(extent))])
    return factor_of


def gaussian(key, dims, spread, reach, pieces=(), kind=jnp.bfloat16):
    gain = steps_of(key, dims, pieces, -0.22, 0.18) if pieces else 1.0
    array = jax.random.normal(key, dims, jnp.float32) * spread * gain
    return jnp.minimum(jnp.maximum(array, -reach), reach).astype(kind)


def setup_inputs(seed: int = 0) -> dict:
    seeds = jax.random.split(jax.random.key(seed), 3)
    source = gaussian(seeds[0], (NT, NZ, 2, SPINS, COLORS, RHS, SITES), 1.0, 6.0, ((0, 8), (1, 4)))
    gauge_field = gaussian(seeds[1], (NT, NZ, 4, 2, COLORS, COLORS, SITES), 0.4, 2.5, ((0, 8), (1, 4)))
    return dict(source=source, gauge_field=gauge_field)


HOPPING = 0.124
GAMMA_PERM = ((3, 2, 1, 0), (3, 2, 1, 0), (2, 3, 0, 1), (2, 3, 0, 1))
GAMMA_PHASE = (((0, 1), (0, 1), (0, -1), (0, -1)),
               ((-1, 0), (1, 0), (1, 0), (-1, 0)),
               ((0, 1), (0, -1), (0, -1), (0, 1)),
               ((1, 0), (1, 0), (1, 0), (1, 0)))


def project(spinor, direction, hop_sign):
    real_part = spinor[..., 0, :, :, :, :].astype(jnp.float32)
    imag_part = spinor[..., 1, :, :, :, :].astype(jnp.float32)
    upper_real = []
    upper_imag = []
    for spin_row in range(2):
        partner = GAMMA_PERM[direction][spin_row]
        phase_re, phase_im = GAMMA_PHASE[direction][spin_row]
        mixed_re = phase_re * real_part[..., partner, :, :, :] - phase_im * imag_part[..., partner, :, :, :]
        mixed_im = phase_re * imag_part[..., partner, :, :, :] + phase_im * real_part[..., partner, :, :, :]
        upper_real.append(real_part[..., spin_row, :, :, :] - hop_sign * mixed_re)
        upper_imag.append(imag_part[..., spin_row, :, :, :] - hop_sign * mixed_im)
    stacked = jnp.stack([jnp.stack(upper_real, -4), jnp.stack(upper_imag, -4)], -5)
    return stacked.astype(jnp.bfloat16)


def color_product(link_field, half_spin, adjoint):
    link_re = link_field[..., 0, :, :, :].astype(jnp.float32)
    link_im = link_field[..., 1, :, :, :].astype(jnp.float32)
    if adjoint:
        link_re = jnp.swapaxes(link_re, -3, -2)
        link_im = -jnp.swapaxes(link_im, -3, -2)
    half_re = half_spin[..., 0, :, :, :, :].astype(jnp.float32)
    half_im = half_spin[..., 1, :, :, :, :].astype(jnp.float32)
    total_re = None
    total_im = None
    for column in range(3):
        mat_re = link_re[..., None, :, column, None, :]
        mat_im = link_im[..., None, :, column, None, :]
        vec_re = half_re[..., :, None, column, :, :]
        vec_im = half_im[..., :, None, column, :, :]
        term_re = mat_re * vec_re - mat_im * vec_im
        term_im = mat_re * vec_im + mat_im * vec_re
        total_re = term_re if total_re is None else total_re + term_re
        total_im = term_im if total_im is None else total_im + term_im
    return jnp.stack([total_re, total_im], -5)


def rebuild(product, direction, hop_sign):
    prod_re = product[..., 0, :, :, :, :]
    prod_im = product[..., 1, :, :, :, :]
    rows_re = [prod_re[..., 0, :, :, :], prod_re[..., 1, :, :, :]]
    rows_im = [prod_im[..., 0, :, :, :], prod_im[..., 1, :, :, :]]
    for spin_row in (2, 3):
        partner = GAMMA_PERM[direction][spin_row]
        phase_re, phase_im = GAMMA_PHASE[direction][spin_row]
        rows_re.append(-hop_sign * (phase_re * prod_re[..., partner, :, :, :] - phase_im * prod_im[..., partner, :, :, :]))
        rows_im.append(-hop_sign * (phase_re * prod_im[..., partner, :, :, :] + phase_im * prod_re[..., partner, :, :, :]))
    return jnp.stack([jnp.stack(rows_re, -4), jnp.stack(rows_im, -4)], -5)


def space_roll(values, direction, amount):
    full_shape = values.shape
    plane_grid = values.reshape(full_shape[:-1] + (NY, NX))
    rolled = jnp.roll(plane_grid, amount, axis=(-1 if direction == 0 else -2))
    return rolled.reshape(full_shape)


def space_hops(spinor, link_all):
    hop_sum = None
    for direction in (0, 1):
        link_field = link_all[..., direction, :, :, :, :]
        ahead_half = space_roll(project(spinor, direction, 1), direction, -1)
        term = rebuild(color_product(link_field, ahead_half, False), direction, 1)
        hop_sum = term if hop_sum is None else hop_sum + term
        behind = color_product(link_field, project(spinor, direction, -1), True)
        hop_sum = hop_sum + rebuild(space_roll(behind, direction, 1), direction, -1)
    return hop_sum


def apply_all(spinor, gauge_field):
    time_count = spinor.shape[0]

    def one_slice(slice_index):
        before_index = (slice_index - 1) % time_count
        after_index = (slice_index + 1) % time_count
        current = spinor[slice_index]
        links_now = gauge_field[slice_index]
        hop_sum = space_hops(current, links_now)
        ahead_half = jnp.roll(project(current, 2, 1), -1, axis=0)
        hop_sum = hop_sum + rebuild(color_product(links_now[:, 2], ahead_half, False), 2, 1)
        behind = jnp.roll(color_product(links_now[:, 2], project(current, 2, -1), True), 1, axis=0)
        hop_sum = hop_sum + rebuild(behind, 2, -1)
        forward_sign = jnp.where(slice_index == time_count - 1, -1.0, 1.0).astype(jnp.float32)
        backward_sign = jnp.where(slice_index == 0, -1.0, 1.0).astype(jnp.float32)
        ahead_time = project(spinor[after_index], 3, 1)
        hop_sum = hop_sum + rebuild(color_product(links_now[:, 3], ahead_time, False) * forward_sign, 3, 1)
        links_before = gauge_field[before_index][:, 3]
        behind_time = color_product(links_before, project(spinor[before_index], 3, -1), True) * backward_sign
        hop_sum = hop_sum + rebuild(behind_time, 3, -1)
        return (current.astype(jnp.float32) - HOPPING * hop_sum).astype(jnp.bfloat16)

    return lax.map(one_slice, jnp.arange(time_count, dtype=jnp.int32))


def reference(source, gauge_field):
    first_pass = apply_all(source, gauge_field)
    return apply_all(first_pass, gauge_field)
```

```python
import functools

import jax
import jax.numpy as jnp
from jax import lax
from jax.experimental import pallas as pl
from jax.experimental.pallas import tpu as pltpu
from jax.sharding import PartitionSpec as P

NX = 16
HOPPING = 0.124
GAMMA_PERM = ((3, 2, 1, 0), (3, 2, 1, 0), (2, 3, 0, 1), (2, 3, 0, 1))
GAMMA_PHASE = (
    ((0, 1), (0, 1), (0, -1), (0, -1)),
    ((-1, 0), (1, 0), (1, 0), (-1, 0)),
    ((0, 1), (0, -1), (0, -1), (0, 1)),
    ((1, 0), (1, 0), (1, 0), (1, 0)),
)
LANES = 128
MESH = pl.DeviceIdType.MESH
COMPONENTS = [(ri, s, c) for ri in range(2) for s in range(4) for c in range(3)]

HALOS = ((3, 1), (3, -1), (2, 1), (2, -1))


def signed_sum(base, term, sign):
    return base + term if sign > 0 else base - term


def project_row(psi, direction, hop_sign, s):
    partner = GAMMA_PERM[direction][s]
    pr, pi = GAMMA_PHASE[direction][s]
    row = []
    for c in range(3):
        if pi == 0:
            re = signed_sum(psi(0, s, c), psi(0, partner, c), -hop_sign * pr)
            im = signed_sum(psi(1, s, c), psi(1, partner, c), -hop_sign * pr)
        else:
            re = signed_sum(psi(0, s, c), psi(1, partner, c), hop_sign * pi)
            im = signed_sum(psi(1, s, c), psi(0, partner, c), -hop_sign * pi)
        row.append((re, im))
    return row


def color_product(link, row):
    out = []
    for r in range(3):
        re = im = None
        for c in range(3):
            lr, li = link(0, r, c), link(1, r, c)
            hr, hi = row[c]
            tr = lr * hr - li * hi
            ti = lr * hi + li * hr
            re = tr if re is None else re + tr
            im = ti if im is None else im + ti
        out.append((re, im))
    return out


def add_rebuilt(total, row, direction, hop_sign, s):
    low = GAMMA_PERM[direction].index(s)
    pr, pi = GAMMA_PHASE[direction][low]
    for c in range(3):
        kr, ki = row[c]
        total[0, s, c] = total[0, s, c] + kr
        total[1, s, c] = total[1, s, c] + ki
        if pi == 0:
            total[0, low, c] = signed_sum(total[0, low, c], kr, -hop_sign * pr)
            total[1, low, c] = signed_sum(total[1, low, c], ki, -hop_sign * pr)
        else:
            total[0, low, c] = signed_sum(total[0, low, c], ki, hop_sign * pi)
            total[1, low, c] = signed_sum(total[1, low, c], kr, -hop_sign * pi)


def packed(pair):
    return jnp.concatenate(pair, 0).astype(jnp.bfloat16)


def widened(tile):
    wide = tile.astype(jnp.float32)
    return wide[:8], wide[8:]


def shift_sites(tile, direction, steps):
    lane = lax.broadcasted_iota(jnp.int32, (8, LANES), 1)
    if direction == 0:
        column = lane % NX
        if steps > 0:
            return jnp.where(
                column == NX - 1,
                pltpu.roll(tile, NX - 1, axis=1),
                pltpu.roll(tile, LANES - 1, axis=1),
            )
        return jnp.where(
            column == 0,
            pltpu.roll(tile, LANES - (NX - 1), axis=1),
            pltpu.roll(tile, 1, axis=1),
        )
    near = pltpu.roll(tile, LANES - NX if steps > 0 else NX, axis=1)
    first_half = lax.broadcasted_iota(jnp.int32, (8, LANES), 0) % 2 == 0
    other = jnp.where(first_half, pltpu.roll(near, 7, axis=0), pltpu.roll(near, 1, axis=0))
    return jnp.where(lane >= LANES - NX if steps > 0 else lane < NX, other, near)


def plane(ri, s, c):
    return (ri * 4 + s) * 3 + c


def link_slot(direction, hop_sign):
    return direction * 2 + (0 if hop_sign > 0 else 1)


def kernel(
    groups, source_hbm, gauge_hbm, out, source, gauge, wide, psi, acc, links, sent, got,
    load_sem, send_sem, stage_sem, final_sem, ready,
):
    chunks = 2 * groups
    ta, gz = lax.axis_index("ta"), lax.axis_index("gz")
    nt, nz = lax.axis_size("ta"), lax.axis_size("gz")
    above_t = (lax.rem(ta + 1, nt), gz)
    below_t = (lax.rem(ta + nt - 1, nt), gz)
    above_z = (ta, lax.rem(gz + 1, nz))
    below_z = (ta, lax.rem(gz + nz - 1, nz))
    targets = (below_t, above_t, below_z, above_z)

    gauge_load = pltpu.make_async_copy(gauge_hbm, gauge, load_sem.at[0])
    source_load = pltpu.make_async_copy(source_hbm, source, load_sem.at[1])
    gauge_load.start()
    source_load.start()

    barrier = pltpu.get_barrier_semaphore()

    def signal_when(condition, semaphore, target):
        @pl.when(condition)
        def _():
            pl.semaphore_signal(semaphore, inc=1, device_id=target, device_id_type=MESH)

    def wait_for(semaphore, *conditions):
        count = sum(c.astype(jnp.int32) for c in conditions)

        @pl.when(count > 0)
        def _():
            pl.semaphore_wait(semaphore, count)

    first_t, last_t, first_z, last_z = ta == 0, ta == nt - 1, gz == 0, gz == nz - 1
    signal_when(ta < nt - 1, barrier, above_t)
    signal_when(first_t, barrier, below_t)
    signal_when(gz < nz - 1, barrier, above_z)
    signal_when(first_z, barrier, below_z)
    wait_for(barrier, ta > 0, last_t, gz > 0, last_z)
    signal_when(last_z, ready.at[2], above_z)
    signal_when(gz > 0, ready.at[1], below_z)
    signal_when(ta > 0, ready.at[0], below_t)
    signal_when(last_t, ready.at[0], above_t)

    upper = (2 * gz) // nz

    def is_late(halo):
        there = (2 * lax.rem(gz + (nz - 1 if halo == 2 else 1), nz)) // nz
        return there if halo == 2 else 1 - there

    def start_halo(step, halo, q):
        if step == 1:
            slot, semaphore = halo, final_sem.at[q]
        elif halo < 2:
            slot, semaphore = halo, stage_sem.at[0, q]
        else:
            late = is_late(halo)
            slot, semaphore = 2 + late, stage_sem.at[late, q]
        pltpu.make_async_remote_copy(
            src_ref=sent.at[step, halo, q],
            dst_ref=got.at[step, q, slot],
            send_sem=send_sem.at[0],
            recv_sem=semaphore,
            device_id=targets[halo],
            device_id_type=MESH,
        ).start()

    def start_all(*halos):
        def one(q, carry):
            for condition, halo in halos:
                @pl.when(condition)
                def _():
                    start_halo(0, halo, q)
            return carry

        lax.fori_loop(0, chunks, one, 0)

    def landed(ref, semaphore):
        return pltpu.make_async_remote_copy(
            src_ref=ref, dst_ref=ref, send_sem=send_sem.at[0], recv_sem=semaphore,
            device_id=above_t, device_id_type=MESH,
        )

    def load_link(direction, hop_sign):
        slot = link_slot(direction, hop_sign)
        return lambda ri, r, c: links[slot, ri * 9 + r * 3 + c]

    def put_halo(step, halo, q, s, at):
        direction, hop_sign = HALOS[halo]
        row = project_row(at, direction, hop_sign, s)
        if hop_sign < 0:
            row = color_product(load_link(direction, -1), row)
        for c in range(3):
            sent[step, halo, q, 16 * c : 16 * c + 16] = packed(row[c])

    def add_halo(total, step, slot, q, s, halo):
        direction, hop_sign = HALOS[halo]
        row = [widened(got[step, q, slot, 16 * c : 16 * c + 16]) for c in range(3)]
        if hop_sign > 0:
            row = color_product(load_link(direction, 1), row)
        add_rebuilt(total, row, direction, hop_sign, s)

    def rows_of(ri, s, c, g):
        return pl.ds(((ri * 3 + c) * groups + g) * 32 + s, 8, stride=4)

    first_half = lax.broadcasted_iota(jnp.int32, (8, LANES), 0) % 2 == 0

    def spread(rows, ri, scale):
        return scale * jnp.where(
            first_half,
            jnp.broadcast_to(rows[ri : ri + 1], (8, LANES)),
            jnp.broadcast_to(rows[2 + ri : 3 + ri], (8, LANES)),
        )

    def put_links(*directions):
        for direction in directions:
            scale = jnp.float32(-HOPPING)
            if direction == 3:
                scale = jnp.where(last_t, HOPPING, -HOPPING).astype(jnp.float32)
            for r in range(3):
                for c in range(3):
                    rows = gauge[direction * 9 + r * 3 + c].astype(jnp.float32)
                    for ri in range(2):
                        tile = spread(rows, ri, scale)
                        links[link_slot(direction, 1), ri * 9 + r * 3 + c] = tile
                        if direction < 2:
                            tile = shift_sites(tile, direction, -1)
                        links[link_slot(direction, -1), ri * 9 + c * 3 + r] = tile if ri == 0 else -tile

    gauge_load.wait()
    put_links(3, 2)
    source_load.wait()
    for p in range(source.shape[0]):
        wide[8 * p : 8 * p + 8] = source[p].astype(jnp.float32)
    for g in range(groups):
        for ri, s, c in COMPONENTS:
            psi[0, g, plane(ri, s, c)] = wide[rows_of(ri, s, c, g)]

    def load_psi(step, g):
        return lambda ri, s, c: psi[step, g, plane(ri, s, c)]

    def first_halos(g, carry):
        for s in range(2):
            for halo in range(4):
                put_halo(0, halo, 2 * g + s, s, load_psi(0, g))
        return carry

    lax.fori_loop(0, groups, first_halos, 0)
    start_all((last_z, 3), (ta > 0, 0), (last_t, 1))
    start_all((gz > 0, 2))
    wait_for(ready.at[1], gz < nz - 1)
    start_all((gz < nz - 1, 3))
    wait_for(ready.at[0], ta < nt - 1, first_t)
    start_all((ta < nt - 1, 1), (first_t, 0))

    put_links(0, 1)

    def load_acc(g):
        return {at: acc[g, plane(*at)] for at in COMPONENTS}

    def plane_hops(step):
        def body(g, carry):
            at = load_psi(step, g)
            total = {key: at(*key) for key in COMPONENTS}
            for direction in (0, 1):
                for hop_sign in (1, -1):
                    for s in range(2):
                        row = [
                            tuple(shift_sites(v, direction, hop_sign) for v in pair)
                            for pair in project_row(at, direction, hop_sign, s)
                        ]
                        row = color_product(load_link(direction, hop_sign), row)
                        add_rebuilt(total, row, direction, hop_sign, s)
            for key, tile in total.items():
                acc[g, plane(*key)] = tile
            return carry

        lax.fori_loop(0, groups, body, 0)

    plane_hops(0)
    wait_for(ready.at[2], first_z)
    start_all((first_z, 2))

    def stages(near, far):
        def early(g, carry):
            for s in range(2):
                q = 2 * g + s
                total = {k: acc[g, plane(*k)] for k in COMPONENTS if k[1] in (s, s + 2)}
                landed(got.at[0, q, pl.ds(0, 3)], stage_sem.at[0, q]).wait_recv()
                add_halo(total, 0, 0, q, s, 0)
                add_halo(total, 0, 1, q, s, 1)
                add_halo(total, 0, 2, q, s, near)
                put_halo(1, near, q, s, lambda *k: total[k])
                start_halo(1, near, q)
                for k, tile in total.items():
                    acc[g, plane(*k)] = tile
            return carry

        def late(g, carry):
            for s in range(2):
                q = 2 * g + s
                total = {k: acc[g, plane(*k)] for k in COMPONENTS if k[1] in (s, s + 2)}
                landed(got.at[0, q, 3], stage_sem.at[1, q]).wait_recv()
                add_halo(total, 0, 3, q, s, far)
                for s2 in (s, s + 2):
                    for c in range(3):
                        total[0, s2, c], total[1, s2, c] = widened(
                            packed([total[0, s2, c], total[1, s2, c]])
                        )
                for halo in (0, 1, far):
                    put_halo(1, halo, q, s, lambda *k: total[k])
                for halo in (0, 1, far):
                    start_halo(1, halo, q)
                for k, tile in total.items():
                    psi[1, g, plane(*k)] = tile
            return carry

        lax.fori_loop(0, groups, early, 0)
        lax.fori_loop(0, groups, late, 0)

    @pl.when(upper == 0)
    def _():
        stages(2, 3)

    @pl.when(upper == 1)
    def _():
        stages(3, 2)

    plane_hops(1)

    def last(g, carry):
        for s in range(2):
            q = 2 * g + s
            total = {k: acc[g, plane(*k)] for k in COMPONENTS if k[1] in (s, s + 2)}
            landed(got.at[1, q], final_sem.at[q]).wait_recv()
            for halo in range(4):
                add_halo(total, 1, halo, q, s, halo)
            for (ri, s2, c), tile in total.items():
                wide[rows_of(ri, s2, c, g)] = tile
        for block in range(6):
            for p in range(4):
                at = (block * groups + g) * 4 + p
                out[at] = wide[pl.ds(8 * at, 8)].astype(jnp.bfloat16)
        return carry

    lax.fori_loop(0, groups, last, 0)
    landed(sent, stage_sem.at[0, 0]).wait_send()


def body(source, gauge_field):
    rhs = source.shape[5]
    groups = rhs // 4
    chunks = 2 * groups
    source_rows = source.reshape(2, 4, 3, rhs, 2, LANES).transpose(0, 2, 3, 4, 1, 5)
    source_rows = source_rows.reshape(6 * rhs, 8, LANES)
    gauge_rows = gauge_field.reshape(4, 2, 3, 3, 2, LANES).transpose(0, 2, 3, 4, 1, 5)
    gauge_rows = gauge_rows.reshape(36, 4, LANES)
    rows = pl.pallas_call(
        functools.partial(kernel, groups),
        out_shape=pltpu.VMEM(source_rows.shape, source.dtype),
        in_specs=[pl.BlockSpec(memory_space=pltpu.HBM)] * 2,
        out_specs=pl.BlockSpec(memory_space=pltpu.VMEM),
        scratch_shapes=[
            pltpu.VMEM(source_rows.shape, jnp.bfloat16),
            pltpu.VMEM(gauge_rows.shape, jnp.bfloat16),
            pltpu.VMEM((48 * rhs, LANES), jnp.float32),
            pltpu.VMEM((2, groups, 24, 8, LANES), jnp.float32),
            pltpu.VMEM((groups, 24, 8, LANES), jnp.float32),
            pltpu.VMEM((8, 18, 8, LANES), jnp.float32),
            pltpu.VMEM((2, 4, chunks, 48, LANES), jnp.bfloat16),
            pltpu.VMEM((2, chunks, 4, 48, LANES), jnp.bfloat16),
            pltpu.SemaphoreType.DMA((2,)),
            pltpu.SemaphoreType.DMA((1,)),
            pltpu.SemaphoreType.DMA((2, chunks)),
            pltpu.SemaphoreType.DMA((chunks,)),
            pltpu.SemaphoreType.REGULAR((3,)),
        ],
        compiler_params=pltpu.CompilerParams(collective_id=0, has_side_effects=True),
        name="dirac_twice",
    )(source_rows, gauge_rows)
    out = rows.reshape(2, 3, rhs, 2, 4, LANES).transpose(0, 4, 1, 2, 3, 5)
    return out.reshape(source.shape)


def solution(mesh):
    spec = P("ta", "gz", None, None, None, None, None)
    return jax.shard_map(body, mesh=mesh, in_specs=(spec, spec), out_specs=spec, check_vma=False)
```

```python
import functools

import jax
import jax.numpy as jnp
from jax import lax
from jax.experimental import pallas as pl
from jax.experimental.pallas import tpu as pltpu
from jax.sharding import PartitionSpec as P

NX = 16
HOPPING = 0.124
GAMMA_PERM = ((3, 2, 1, 0), (3, 2, 1, 0), (2, 3, 0, 1), (2, 3, 0, 1))
GAMMA_PHASE = (
    ((0, 1), (0, 1), (0, -1), (0, -1)),
    ((-1, 0), (1, 0), (1, 0), (-1, 0)),
    ((0, 1), (0, -1), (0, -1), (0, 1)),
    ((1, 0), (1, 0), (1, 0), (1, 0)),
)
LANES = 128
MESH = pl.DeviceIdType.MESH
COMPONENTS = [(ri, s, c) for ri in range(2) for s in range(4) for c in range(3)]

HALOS = ((3, 1), (3, -1), (2, 1), (2, -1))


def signed_sum(base, term, sign):
    return base + term if sign > 0 else base - term


def project_row(psi, direction, hop_sign, s):
    partner = GAMMA_PERM[direction][s]
    pr, pi = GAMMA_PHASE[direction][s]
    row = []
    for c in range(3):
        if pi == 0:
            re = signed_sum(psi(0, s, c), psi(0, partner, c), -hop_sign * pr)
            im = signed_sum(psi(1, s, c), psi(1, partner, c), -hop_sign * pr)
        else:
            re = signed_sum(psi(0, s, c), psi(1, partner, c), hop_sign * pi)
            im = signed_sum(psi(1, s, c), psi(0, partner, c), -hop_sign * pi)
        row.append((re, im))
    return row


def color_product(link, row):
    out = []
    for r in range(3):
        re = im = None
        for c in range(3):
            lr, li = link(0, r, c), link(1, r, c)
            hr, hi = row[c]
            tr = lr * hr - li * hi
            ti = lr * hi + li * hr
            re = tr if re is None else re + tr
            im = ti if im is None else im + ti
        out.append((re, im))
    return out


def add_rebuilt(total, row, direction, hop_sign, s):
    low = GAMMA_PERM[direction].index(s)
    pr, pi = GAMMA_PHASE[direction][low]
    for c in range(3):
        kr, ki = row[c]
        total[0, s, c] = total[0, s, c] + kr
        total[1, s, c] = total[1, s, c] + ki
        if pi == 0:
            total[0, low, c] = signed_sum(total[0, low, c], kr, -hop_sign * pr)
            total[1, low, c] = signed_sum(total[1, low, c], ki, -hop_sign * pr)
        else:
            total[0, low, c] = signed_sum(total[0, low, c], ki, hop_sign * pi)
            total[1, low, c] = signed_sum(total[1, low, c], kr, -hop_sign * pi)


def packed(pair):
    return jnp.concatenate(pair, 0).astype(jnp.bfloat16)


def widened(tile):
    wide = tile.astype(jnp.float32)
    return wide[:8], wide[8:]


def shift_sites(tile, direction, steps):
    lane = lax.broadcasted_iota(jnp.int32, (8, LANES), 1)
    if direction == 0:
        column = lane % NX
        if steps > 0:
            return jnp.where(
                column == NX - 1,
                pltpu.roll(tile, NX - 1, axis=1),
                pltpu.roll(tile, LANES - 1, axis=1),
            )
        return jnp.where(
            column == 0,
            pltpu.roll(tile, LANES - (NX - 1), axis=1),
            pltpu.roll(tile, 1, axis=1),
        )
    near = pltpu.roll(tile, LANES - NX if steps > 0 else NX, axis=1)
    first_half = lax.broadcasted_iota(jnp.int32, (8, LANES), 0) % 2 == 0
    other = jnp.where(first_half, pltpu.roll(near, 7, axis=0), pltpu.roll(near, 1, axis=0))
    return jnp.where(lane >= LANES - NX if steps > 0 else lane < NX, other, near)


def plane(ri, s, c):
    return (ri * 4 + s) * 3 + c


def link_slot(direction, hop_sign):
    return direction * 2 + (0 if hop_sign > 0 else 1)


def kernel(
    groups, source_hbm, gauge_hbm, out, source, gauge, wide, psi, acc, links, sent, got,
    load_sem, send_sem, stage_sem, final_sem, ready,
):
    chunks = 2 * groups
    ta, gz = lax.axis_index("ta"), lax.axis_index("gz")
    nt, nz = lax.axis_size("ta"), lax.axis_size("gz")
    above_t = (lax.rem(ta + 1, nt), gz)
    below_t = (lax.rem(ta + nt - 1, nt), gz)
    above_z = (ta, lax.rem(gz + 1, nz))
    below_z = (ta, lax.rem(gz + nz - 1, nz))
    targets = (below_t, above_t, below_z, above_z)

    def block_loads(g):
        rows = groups * 4
        return [
            pltpu.make_async_copy(
                source_hbm.at[pl.ds(block * rows + 4 * g, 4)],
                source.at[pl.ds(block * rows + 4 * g, 4)],
                load_sem.at[g],
            )
            for block in range(6)
        ]

    def source_group(g):
        return pltpu.make_async_copy(
            source_hbm.at[pl.ds(0, 24)], source.at[pl.ds(0, 24)], load_sem.at[g]
        )

    far_gauge = pltpu.make_async_copy(
        gauge_hbm.at[pl.ds(18, 18)], gauge.at[pl.ds(18, 18)], load_sem.at[groups]
    )
    near_gauge = pltpu.make_async_copy(
        gauge_hbm.at[pl.ds(0, 18)], gauge.at[pl.ds(0, 18)], load_sem.at[groups + 1]
    )
    far_gauge.start()
    for g in range(groups):
        for load in block_loads(g):
            load.start()
    near_gauge.start()

    barrier = pltpu.get_barrier_semaphore()

    def signal_when(condition, semaphore, target):
        @pl.when(condition)
        def _():
            pl.semaphore_signal(semaphore, inc=1, device_id=target, device_id_type=MESH)

    def wait_for(semaphore, *conditions):
        count = sum(c.astype(jnp.int32) for c in conditions)

        @pl.when(count > 0)
        def _():
            pl.semaphore_wait(semaphore, count)

    first_t, last_t, first_z, last_z = ta == 0, ta == nt - 1, gz == 0, gz == nz - 1
    stands_back = (lax.rem(ta, 2) == 1) & (ta > 1) & ~last_t
    even, odd = lax.rem(ta, 2) == 0, lax.rem(ta, 2) == 1
    met_below_t, met_above_t = (ta > 0) & (ta != nt // 2), last_t | (ta == nt // 2 - 1)
    met_below_z, met_above_z = ~first_z, last_z
    signal_when(~met_above_t, barrier, above_t)
    signal_when(~met_below_t, barrier, below_t)
    signal_when(~met_above_z, barrier, above_z)
    signal_when(~met_below_z, barrier, below_z)
    wait_for(barrier, met_below_t, met_above_t, met_below_z, met_above_z)
    signal_when(met_above_z, ready.at[2], above_z)
    signal_when(met_below_z, ready.at[1], below_z)
    signal_when(met_below_t, ready.at[0], below_t)
    signal_when(met_above_t, ready.at[0], above_t)

    upper = (2 * gz) // nz

    def is_late(halo):
        there = (2 * lax.rem(gz + (nz - 1 if halo == 2 else 1), nz)) // nz
        return there if halo == 2 else 1 - there

    def start_halo(step, halo, q):
        if step == 1:
            slot, semaphore = halo, final_sem.at[q]
        elif halo < 2:
            slot, semaphore = halo, stage_sem.at[0, q]
        else:
            late = is_late(halo)
            slot, semaphore = 2 + late, stage_sem.at[late, q]
        pltpu.make_async_remote_copy(
            src_ref=sent.at[step, halo, q],
            dst_ref=got.at[step, q, slot],
            send_sem=send_sem.at[0],
            recv_sem=semaphore,
            device_id=targets[halo],
            device_id_type=MESH,
        ).start()

    def start_all(*halos, step=0):
        def one(q, carry):
            for condition, halo in halos:
                @pl.when(condition)
                def _():
                    start_halo(step, halo, q)
            return carry

        lax.fori_loop(0, chunks, one, 0)

    def landed(ref, semaphore):
        return pltpu.make_async_remote_copy(
            src_ref=ref, dst_ref=ref, send_sem=send_sem.at[0], recv_sem=semaphore,
            device_id=above_t, device_id_type=MESH,
        )

    def load_link(direction, hop_sign):
        slot = link_slot(direction, hop_sign)
        return lambda ri, r, c: links[slot, ri * 9 + r * 3 + c]

    def put_halo(step, halo, q, s, at):
        direction, hop_sign = HALOS[halo]
        row = project_row(at, direction, hop_sign, s)
        if hop_sign < 0:
            row = color_product(load_link(direction, -1), row)
        for c in range(3):
            sent[step, halo, q, 16 * c : 16 * c + 16] = packed(row[c])

    def add_halo(total, step, slot, q, s, halo):
        direction, hop_sign = HALOS[halo]
        row = [widened(got[step, q, slot, 16 * c : 16 * c + 16]) for c in range(3)]
        if hop_sign > 0:
            row = color_product(load_link(direction, 1), row)
        add_rebuilt(total, row, direction, hop_sign, s)

    def rows_of(ri, s, c, g):
        return pl.ds(((ri * 3 + c) * groups + g) * 32 + s, 8, stride=4)

    first_half = lax.broadcasted_iota(jnp.int32, (8, LANES), 0) % 2 == 0

    def spread(rows, ri, scale):
        return scale * jnp.where(
            first_half,
            jnp.broadcast_to(rows[ri : ri + 1], (8, LANES)),
            jnp.broadcast_to(rows[2 + ri : 3 + ri], (8, LANES)),
        )

    def put_links(*directions):
        for direction in directions:
            scale = jnp.float32(-HOPPING)
            if direction == 3:
                scale = jnp.where(last_t, HOPPING, -HOPPING).astype(jnp.float32)
            for r in range(3):
                for c in range(3):
                    rows = gauge[direction * 9 + r * 3 + c].astype(jnp.float32)
                    for ri in range(2):
                        tile = spread(rows, ri, scale)
                        links[link_slot(direction, 1), ri * 9 + r * 3 + c] = tile
                        if direction < 2:
                            tile = shift_sites(tile, direction, -1)
                        links[link_slot(direction, -1), ri * 9 + c * 3 + r] = tile if ri == 0 else -tile

    def load_psi(step, g):
        return lambda ri, s, c: psi[step, g, plane(ri, s, c)]

    def start_when(condition, halo, g):
        @pl.when(condition)
        def _():
            for s in range(2):
                start_halo(0, halo, 2 * g + s)

    far_gauge.wait()
    put_links(3, 2)
    for g in range(groups):
        source_group(g).wait()
        for block in range(6):
            for p in range(4):
                at = (block * groups + g) * 4 + p
                wide[8 * at : 8 * at + 8] = source[at].astype(jnp.float32)
        tiles = {(ri, s, c): wide[rows_of(ri, s, c, g)] for ri, s, c in COMPONENTS}
        for halo in range(4):
            for s in range(2):
                put_halo(0, halo, 2 * g + s, s, lambda *k: tiles[k])
        for k, tile in tiles.items():
            psi[0, g, plane(*k)] = tile
        start_when(last_z & ~stands_back, 3, g)
        start_when(met_below_t, 0, g)
        start_when(met_above_t, 1, g)
    start_all((met_below_z, 2))
    wait_for(ready.at[1], ~met_above_z)
    start_all((~met_above_z, 3))
    wait_for(ready.at[0], ~met_above_t, ~met_below_t)
    start_all((~met_above_t, 1), (~met_below_t, 0))
    start_all((last_z & stands_back, 3))

    near_gauge.wait()
    put_links(0, 1)

    def load_acc(g):
        return {at: acc[g, plane(*at)] for at in COMPONENTS}

    def plane_hops(step):
        def body(g, carry):
            at = load_psi(step, g)
            total = {key: at(*key) for key in COMPONENTS}
            for direction in (0, 1):
                for hop_sign in (1, -1):
                    for s in range(2):
                        row = [
                            tuple(shift_sites(v, direction, hop_sign) for v in pair)
                            for pair in project_row(at, direction, hop_sign, s)
                        ]
                        row = color_product(load_link(direction, hop_sign), row)
                        add_rebuilt(total, row, direction, hop_sign, s)
            for key, tile in total.items():
                acc[g, plane(*key)] = tile
            return carry

        lax.fori_loop(0, groups, body, 0)

    plane_hops(0)
    wait_for(ready.at[2], first_z)
    start_all((first_z, 2))

    def stages(near, far):
        def early(g, carry):
            for s in range(2):
                q = 2 * g + s
                total = {k: acc[g, plane(*k)] for k in COMPONENTS if k[1] in (s, s + 2)}
                landed(got.at[0, q, pl.ds(0, 3)], stage_sem.at[0, q]).wait_recv()
                add_halo(total, 0, 0, q, s, 0)
                add_halo(total, 0, 1, q, s, 1)
                add_halo(total, 0, 2, q, s, near)
                put_halo(1, near, q, s, lambda *k: total[k])
                start_halo(1, near, q)
                for k, tile in total.items():
                    acc[g, plane(*k)] = tile
            return carry

        def late(g, carry):
            for s in range(2):
                q = 2 * g + s
                total = {k: acc[g, plane(*k)] for k in COMPONENTS if k[1] in (s, s + 2)}
                landed(got.at[0, q, 3], stage_sem.at[1, q]).wait_recv()
                add_halo(total, 0, 3, q, s, far)
                for s2 in (s, s + 2):
                    for c in range(3):
                        total[0, s2, c], total[1, s2, c] = widened(
                            packed([total[0, s2, c], total[1, s2, c]])
                        )
                for halo in (0, 1, far):
                    put_halo(1, halo, q, s, lambda *k: total[k])
                for halo in (0, 1, far):
                    start_halo(1, halo, q)
                for k, tile in total.items():
                    psi[1, g, plane(*k)] = tile
            return carry

        lax.fori_loop(0, groups, early, 0)
        lax.fori_loop(0, groups, late, 0)

    @pl.when(upper == 0)
    def _():
        stages(2, 3)

    @pl.when(upper == 1)
    def _():
        stages(3, 2)

    plane_hops(1)

    def last(g, carry):
        for s in range(2):
            q = 2 * g + s
            total = {k: acc[g, plane(*k)] for k in COMPONENTS if k[1] in (s, s + 2)}
            landed(got.at[1, q], final_sem.at[q]).wait_recv()
            for halo in range(4):
                add_halo(total, 1, halo, q, s, halo)
            for (ri, s2, c), tile in total.items():
                wide[rows_of(ri, s2, c, g)] = tile
        for block in range(6):
            for p in range(4):
                at = (block * groups + g) * 4 + p
                out[at] = wide[pl.ds(8 * at, 8)].astype(jnp.bfloat16)
        return carry

    lax.fori_loop(0, groups, last, 0)
    landed(sent, stage_sem.at[0, 0]).wait_send()


def body(source, gauge_field):
    rhs = source.shape[5]
    groups = rhs // 4
    chunks = 2 * groups
    source_rows = source.reshape(2, 4, 3, rhs, 2, LANES).transpose(0, 2, 3, 4, 1, 5)
    source_rows = source_rows.reshape(6 * rhs, 8, LANES)
    gauge_rows = gauge_field.reshape(4, 2, 3, 3, 2, LANES).transpose(0, 2, 3, 4, 1, 5)
    gauge_rows = gauge_rows.reshape(36, 4, LANES)
    rows = pl.pallas_call(
        functools.partial(kernel, groups),
        out_shape=pltpu.VMEM(source_rows.shape, source.dtype),
        in_specs=[pl.BlockSpec(memory_space=pltpu.HBM)] * 2,
        out_specs=pl.BlockSpec(memory_space=pltpu.VMEM),
        scratch_shapes=[
            pltpu.VMEM(source_rows.shape, jnp.bfloat16),
            pltpu.VMEM(gauge_rows.shape, jnp.bfloat16),
            pltpu.VMEM((48 * rhs, LANES), jnp.float32),
            pltpu.VMEM((2, groups, 24, 8, LANES), jnp.float32),
            pltpu.VMEM((groups, 24, 8, LANES), jnp.float32),
            pltpu.VMEM((8, 18, 8, LANES), jnp.float32),
            pltpu.VMEM((2, 4, chunks, 48, LANES), jnp.bfloat16),
            pltpu.VMEM((2, chunks, 4, 48, LANES), jnp.bfloat16),
            pltpu.SemaphoreType.DMA((groups + 2,)),
            pltpu.SemaphoreType.DMA((1,)),
            pltpu.SemaphoreType.DMA((2, chunks)),
            pltpu.SemaphoreType.DMA((chunks,)),
            pltpu.SemaphoreType.REGULAR((3,)),
        ],
        compiler_params=pltpu.CompilerParams(collective_id=0, has_side_effects=True),
        name="dirac_twice",
    )(source_rows, gauge_rows)
    out = rows.reshape(2, 3, rhs, 2, 4, LANES).transpose(0, 4, 1, 2, 3, 5)
    return out.reshape(source.shape)


def solution(mesh):
    spec = P("ta", "gz", None, None, None, None, None)
    return jax.shard_map(body, mesh=mesh, in_specs=(spec, spec), out_specs=spec, check_vma=False)
```

```python
import functools

import jax
import jax.numpy as jnp
from jax import lax
from jax.experimental import pallas as pl
from jax.experimental.pallas import tpu as pltpu
from jax.sharding import PartitionSpec as P

NX = 16
HOPPING = 0.124
GAMMA_PERM = ((3, 2, 1, 0), (3, 2, 1, 0), (2, 3, 0, 1), (2, 3, 0, 1))
GAMMA_PHASE = (
    ((0, 1), (0, 1), (0, -1), (0, -1)),
    ((-1, 0), (1, 0), (1, 0), (-1, 0)),
    ((0, 1), (0, -1), (0, -1), (0, 1)),
    ((1, 0), (1, 0), (1, 0), (1, 0)),
)
LANES = 128
MESH = pl.DeviceIdType.MESH
COMPONENTS = [(ri, s, c) for ri in range(2) for s in range(4) for c in range(3)]

HALOS = ((3, 1), (3, -1), (2, 1), (2, -1))


def signed_sum(base, term, sign):
    return base + term if sign > 0 else base - term


def project_row(psi, direction, hop_sign, s):
    partner = GAMMA_PERM[direction][s]
    pr, pi = GAMMA_PHASE[direction][s]
    row = []
    for c in range(3):
        if pi == 0:
            re = signed_sum(psi(0, s, c), psi(0, partner, c), -hop_sign * pr)
            im = signed_sum(psi(1, s, c), psi(1, partner, c), -hop_sign * pr)
        else:
            re = signed_sum(psi(0, s, c), psi(1, partner, c), hop_sign * pi)
            im = signed_sum(psi(1, s, c), psi(0, partner, c), -hop_sign * pi)
        row.append((re, im))
    return row


def color_product(link, row):
    out = []
    for r in range(3):
        re = im = None
        for c in range(3):
            lr, li = link(0, r, c), link(1, r, c)
            hr, hi = row[c]
            tr = lr * hr - li * hi
            ti = lr * hi + li * hr
            re = tr if re is None else re + tr
            im = ti if im is None else im + ti
        out.append((re, im))
    return out


def add_rebuilt(total, row, direction, hop_sign, s):
    low = GAMMA_PERM[direction].index(s)
    pr, pi = GAMMA_PHASE[direction][low]
    for c in range(3):
        kr, ki = row[c]
        total[0, s, c] = total[0, s, c] + kr
        total[1, s, c] = total[1, s, c] + ki
        if pi == 0:
            total[0, low, c] = signed_sum(total[0, low, c], kr, -hop_sign * pr)
            total[1, low, c] = signed_sum(total[1, low, c], ki, -hop_sign * pr)
        else:
            total[0, low, c] = signed_sum(total[0, low, c], ki, hop_sign * pi)
            total[1, low, c] = signed_sum(total[1, low, c], kr, -hop_sign * pi)


def packed(pair):
    return jnp.concatenate(pair, 0).astype(jnp.bfloat16)


def widened(tile):
    wide = tile.astype(jnp.float32)
    return wide[:8], wide[8:]


def shift_sites(tile, direction, steps):
    lane = lax.broadcasted_iota(jnp.int32, (8, LANES), 1)
    if direction == 0:
        column = lane % NX
        if steps > 0:
            return jnp.where(
                column == NX - 1,
                pltpu.roll(tile, NX - 1, axis=1),
                pltpu.roll(tile, LANES - 1, axis=1),
            )
        return jnp.where(
            column == 0,
            pltpu.roll(tile, LANES - (NX - 1), axis=1),
            pltpu.roll(tile, 1, axis=1),
        )
    near = pltpu.roll(tile, LANES - NX if steps > 0 else NX, axis=1)
    first_half = lax.broadcasted_iota(jnp.int32, (8, LANES), 0) % 2 == 0
    other = jnp.where(first_half, pltpu.roll(near, 7, axis=0), pltpu.roll(near, 1, axis=0))
    return jnp.where(lane >= LANES - NX if steps > 0 else lane < NX, other, near)


def plane(ri, s, c):
    return (ri * 4 + s) * 3 + c


def link_slot(direction, hop_sign):
    return direction * 2 + (0 if hop_sign > 0 else 1)


def kernel(
    groups, source_hbm, gauge_hbm, out, source, gauge, wide, psi, acc, links, sent, got,
    send_sem, final_sem,
):
    chunks = 2 * groups
    ta, gz = lax.axis_index("ta"), lax.axis_index("gz")
    nt, nz = lax.axis_size("ta"), lax.axis_size("gz")
    above_t = (lax.rem(ta + 1, nt), gz)
    below_t = (lax.rem(ta + nt - 1, nt), gz)
    above_z = (ta, lax.rem(gz + 1, nz))
    below_z = (ta, lax.rem(gz + nz - 1, nz))
    targets = (below_t, above_t, below_z, above_z)

    def landed(ref, semaphore):
        return pltpu.make_async_remote_copy(
            src_ref=ref, dst_ref=ref, send_sem=send_sem.at[0], recv_sem=semaphore,
            device_id=above_t, device_id_type=MESH,
        )

    def load_link(direction, hop_sign):
        slot = link_slot(direction, hop_sign)
        return lambda ri, r, c: links[slot, ri * 9 + r * 3 + c]

    def add_halo(total, step, slot, q, s, halo):
        direction, hop_sign = HALOS[halo]
        row = [widened(got[step, q, slot, 16 * c : 16 * c + 16]) for c in range(3)]
        if hop_sign > 0:
            row = color_product(load_link(direction, 1), row)
        add_rebuilt(total, row, direction, hop_sign, s)

    def rows_of(ri, s, c, g):
        return pl.ds(((ri * 3 + c) * groups + g) * 32 + s, 8, stride=4)

    def load_psi(step, g):
        return lambda ri, s, c: psi[step, g, plane(ri, s, c)]

    def plane_hops(step):
        def body(g, carry):
            at = load_psi(step, g)
            total = {key: at(*key) for key in COMPONENTS}
            for direction in (0, 1):
                for hop_sign in (1, -1):
                    for s in range(2):
                        row = [
                            tuple(shift_sites(v, direction, hop_sign) for v in pair)
                            for pair in project_row(at, direction, hop_sign, s)
                        ]
                        row = color_product(load_link(direction, hop_sign), row)
                        add_rebuilt(total, row, direction, hop_sign, s)
            for key, tile in total.items():
                acc[g, plane(*key)] = tile
            return carry

        lax.fori_loop(0, groups, body, 0)

    def first_application(load_sem, stage_sem, ready):
        def block_loads(g):
            rows = groups * 4
            return [
                pltpu.make_async_copy(
                    source_hbm.at[pl.ds(block * rows + 4 * g, 4)],
                    source.at[pl.ds(block * rows + 4 * g, 4)],
                    load_sem.at[g],
                )
                for block in range(6)
            ]

        def source_group(g):
            return pltpu.make_async_copy(
                source_hbm.at[pl.ds(0, 24)], source.at[pl.ds(0, 24)], load_sem.at[g]
            )

        far_gauge = pltpu.make_async_copy(
            gauge_hbm.at[pl.ds(18, 18)], gauge.at[pl.ds(18, 18)], load_sem.at[groups]
        )
        near_gauge = pltpu.make_async_copy(
            gauge_hbm.at[pl.ds(0, 18)], gauge.at[pl.ds(0, 18)], load_sem.at[groups + 1]
        )
        far_gauge.start()
        for g in range(groups):
            for load in block_loads(g):
                load.start()
        near_gauge.start()

        barrier = pltpu.get_barrier_semaphore()

        def signal_when(condition, semaphore, target):
            @pl.when(condition)
            def _():
                pl.semaphore_signal(semaphore, inc=1, device_id=target, device_id_type=MESH)

        def wait_for(semaphore, *conditions):
            count = sum(c.astype(jnp.int32) for c in conditions)

            @pl.when(count > 0)
            def _():
                pl.semaphore_wait(semaphore, count)

        first_t, last_t, first_z, last_z = ta == 0, ta == nt - 1, gz == 0, gz == nz - 1
        stands_back = (lax.rem(ta, 2) == 1) & (ta > 1) & ~last_t
        even, odd = lax.rem(ta, 2) == 0, lax.rem(ta, 2) == 1
        met_below_t, met_above_t = (ta > 0) & (ta != nt // 2), last_t | (ta == nt // 2 - 1)
        met_below_z, met_above_z = ~first_z, last_z
        signal_when(~met_above_t, barrier, above_t)
        signal_when(~met_below_t, barrier, below_t)
        signal_when(~met_above_z, barrier, above_z)
        signal_when(~met_below_z, barrier, below_z)
        wait_for(barrier, met_below_t, met_above_t, met_below_z, met_above_z)
        signal_when(met_above_z, ready.at[2], above_z)
        signal_when(met_below_z, ready.at[1], below_z)
        signal_when(met_below_t, ready.at[0], below_t)
        signal_when(met_above_t, ready.at[0], above_t)

        upper = (2 * gz) // nz

        def is_late(halo):
            there = (2 * lax.rem(gz + (nz - 1 if halo == 2 else 1), nz)) // nz
            return there if halo == 2 else 1 - there

        def start_halo(step, halo, q):
            if step == 1:
                slot, semaphore = halo, final_sem.at[jnp.maximum(q - (chunks - 3), 0)]
            elif halo < 2:
                slot, semaphore = halo, stage_sem.at[0, q]
            else:
                late = is_late(halo)
                slot, semaphore = 2 + late, stage_sem.at[late, q]
            pltpu.make_async_remote_copy(
                src_ref=sent.at[step, halo, q],
                dst_ref=got.at[step, q, slot],
                send_sem=send_sem.at[0],
                recv_sem=semaphore,
                device_id=targets[halo],
                device_id_type=MESH,
            ).start()

        def start_all(*halos, step=0):
            def one(q, carry):
                for condition, halo in halos:
                    @pl.when(condition)
                    def _():
                        start_halo(step, halo, q)
                return carry

            lax.fori_loop(0, chunks, one, 0)

        def put_halo(step, halo, q, s, at):
            direction, hop_sign = HALOS[halo]
            row = project_row(at, direction, hop_sign, s)
            if hop_sign < 0:
                row = color_product(load_link(direction, -1), row)
            for c in range(3):
                sent[step, halo, q, 16 * c : 16 * c + 16] = packed(row[c])

        first_half = lax.broadcasted_iota(jnp.int32, (8, LANES), 0) % 2 == 0

        def spread(rows, ri, scale):
            return scale * jnp.where(
                first_half,
                jnp.broadcast_to(rows[ri : ri + 1], (8, LANES)),
                jnp.broadcast_to(rows[2 + ri : 3 + ri], (8, LANES)),
            )

        def put_links(*directions):
            for direction in directions:
                scale = jnp.float32(-HOPPING)
                if direction == 3:
                    scale = jnp.where(last_t, HOPPING, -HOPPING).astype(jnp.float32)
                for r in range(3):
                    for c in range(3):
                        rows = gauge[direction * 9 + r * 3 + c].astype(jnp.float32)
                        for ri in range(2):
                            tile = spread(rows, ri, scale)
                            links[link_slot(direction, 1), ri * 9 + r * 3 + c] = tile
                            if direction < 2:
                                tile = shift_sites(tile, direction, -1)
                            links[link_slot(direction, -1), ri * 9 + c * 3 + r] = tile if ri == 0 else -tile

        def start_when(condition, halo, g):
            @pl.when(condition)
            def _():
                for s in range(2):
                    start_halo(0, halo, 2 * g + s)

        far_gauge.wait()
        put_links(3, 2)
        for g in range(groups):
            source_group(g).wait()
            for block in range(6):
                for p in range(4):
                    at = (block * groups + g) * 4 + p
                    wide[8 * at : 8 * at + 8] = source[at].astype(jnp.float32)
            tiles = {(ri, s, c): wide[rows_of(ri, s, c, g)] for ri, s, c in COMPONENTS}
            for halo in range(4):
                for s in range(2):
                    put_halo(0, halo, 2 * g + s, s, lambda *k: tiles[k])
            for k, tile in tiles.items():
                psi[0, g, plane(*k)] = tile
            start_when(last_z & ~stands_back, 3, g)
            start_when(met_below_z & ~last_z, 2, g)
            start_when(met_below_t, 0, g)
            start_when(met_above_t, 1, g)
        start_all((last_z, 2))
        wait_for(ready.at[1], ~met_above_z)
        start_all((~met_above_z, 3))
        wait_for(ready.at[0], ~met_above_t, ~met_below_t)
        start_all((~met_above_t, 1), (~met_below_t, 0))
        start_all((last_z & stands_back, 3))

        near_gauge.wait()
        put_links(0, 1)

        plane_hops(0)
        wait_for(ready.at[2], first_z)
        start_all((first_z, 2))

        def stages(near, far):
            def early(g, carry):
                for s in range(2):
                    q = 2 * g + s
                    total = {k: acc[g, plane(*k)] for k in COMPONENTS if k[1] in (s, s + 2)}
                    landed(got.at[0, q, pl.ds(0, 3)], stage_sem.at[0, q]).wait_recv()
                    add_halo(total, 0, 0, q, s, 0)
                    add_halo(total, 0, 1, q, s, 1)
                    add_halo(total, 0, 2, q, s, near)
                    put_halo(1, near, q, s, lambda *k: total[k])
                    start_halo(1, near, q)
                    for k, tile in total.items():
                        acc[g, plane(*k)] = tile
                return carry

            def late(g, carry):
                for s in range(2):
                    q = 2 * g + s
                    total = {k: acc[g, plane(*k)] for k in COMPONENTS if k[1] in (s, s + 2)}
                    landed(got.at[0, q, 3], stage_sem.at[1, q]).wait_recv()
                    add_halo(total, 0, 3, q, s, far)
                    for s2 in (s, s + 2):
                        for c in range(3):
                            total[0, s2, c], total[1, s2, c] = widened(
                                packed([total[0, s2, c], total[1, s2, c]])
                            )
                    for halo in (0, 1, far):
                        put_halo(1, halo, q, s, lambda *k: total[k])
                    for halo in (0, 1, far):
                        start_halo(1, halo, q)
                    for k, tile in total.items():
                        psi[1, g, plane(*k)] = tile
                return carry

            lax.fori_loop(0, groups, early, 0)
            lax.fori_loop(0, groups, late, 0)

        @pl.when(upper == 0)
        def _():
            stages(2, 3)

        @pl.when(upper == 1)
        def _():
            stages(3, 2)

    pl.run_scoped(
        first_application,
        pltpu.SemaphoreType.DMA((groups + 2,)),
        pltpu.SemaphoreType.DMA((2, chunks)),
        pltpu.SemaphoreType.REGULAR((3,)),
    )
    plane_hops(1)

    for g in range(groups):
        for s in range(2):
            q = 2 * g + s
            total = {k: acc[g, plane(*k)] for k in COMPONENTS if k[1] in (s, s + 2)}
            if q == 0:
                landed(got.at[1, pl.ds(0, chunks - 2)], final_sem.at[0]).wait_recv()
            elif q > chunks - 3:
                landed(got.at[1, q], final_sem.at[q - (chunks - 3)]).wait_recv()
            for halo in range(4):
                add_halo(total, 1, halo, q, s, halo)
            for (ri, s2, c), tile in total.items():
                wide[rows_of(ri, s2, c, g)] = tile
        for block in range(6):
            for p in range(4):
                at = (block * groups + g) * 4 + p
                out[at] = wide[pl.ds(8 * at, 8)].astype(jnp.bfloat16)
    landed(sent, final_sem.at[0]).wait_send()


def body(source, gauge_field):
    rhs = source.shape[5]
    groups = rhs // 4
    chunks = 2 * groups
    source_rows = source.reshape(2, 4, 3, rhs, 2, LANES).transpose(0, 2, 3, 4, 1, 5)
    source_rows = source_rows.reshape(6 * rhs, 8, LANES)
    gauge_rows = gauge_field.reshape(4, 2, 3, 3, 2, LANES).transpose(0, 2, 3, 4, 1, 5)
    gauge_rows = gauge_rows.reshape(36, 4, LANES)
    rows = pl.pallas_call(
        functools.partial(kernel, groups),
        out_shape=pltpu.VMEM(source_rows.shape, source.dtype),
        in_specs=[pl.BlockSpec(memory_space=pltpu.HBM)] * 2,
        out_specs=pl.BlockSpec(memory_space=pltpu.VMEM),
        scratch_shapes=[
            pltpu.VMEM(source_rows.shape, jnp.bfloat16),
            pltpu.VMEM(gauge_rows.shape, jnp.bfloat16),
            pltpu.VMEM((48 * rhs, LANES), jnp.float32),
            pltpu.VMEM((2, groups, 24, 8, LANES), jnp.float32),
            pltpu.VMEM((groups, 24, 8, LANES), jnp.float32),
            pltpu.VMEM((8, 18, 8, LANES), jnp.float32),
            pltpu.VMEM((2, 4, chunks, 48, LANES), jnp.bfloat16),
            pltpu.VMEM((2, chunks, 4, 48, LANES), jnp.bfloat16),
            pltpu.SemaphoreType.DMA((1,)),
            pltpu.SemaphoreType.DMA((3,)),
        ],
        compiler_params=pltpu.CompilerParams(collective_id=0, has_side_effects=True),
        name="dirac_twice",
    )(source_rows, gauge_rows)
    out = rows.reshape(2, 3, rhs, 2, 4, LANES).transpose(0, 4, 1, 2, 3, 5)
    return out.reshape(source.shape)


def solution(mesh):
    spec = P("ta", "gz", None, None, None, None, None)
    return jax.shard_map(body, mesh=mesh, in_specs=(spec, spec), out_specs=spec, check_vma=False)
```

```python
import functools

import jax
import jax.numpy as jnp
from jax import lax
from jax.experimental import pallas as pl
from jax.experimental.pallas import tpu as pltpu
from jax.sharding import PartitionSpec as P

NX = 16
HOPPING = 0.124
GAMMA_PERM = ((3, 2, 1, 0), (3, 2, 1, 0), (2, 3, 0, 1), (2, 3, 0, 1))
GAMMA_PHASE = (
    ((0, 1), (0, 1), (0, -1), (0, -1)),
    ((-1, 0), (1, 0), (1, 0), (-1, 0)),
    ((0, 1), (0, -1), (0, -1), (0, 1)),
    ((1, 0), (1, 0), (1, 0), (1, 0)),
)
LANES = 128
MESH = pl.DeviceIdType.MESH
COMPONENTS = [(ri, s, c) for ri in range(2) for s in range(4) for c in range(3)]

HALOS = ((3, 1), (3, -1), (2, 1), (2, -1))


def signed_sum(base, term, sign):
    return base + term if sign > 0 else base - term


def project_row(psi, direction, hop_sign, s):
    partner = GAMMA_PERM[direction][s]
    pr, pi = GAMMA_PHASE[direction][s]
    row = []
    for c in range(3):
        if pi == 0:
            re = signed_sum(psi(0, s, c), psi(0, partner, c), -hop_sign * pr)
            im = signed_sum(psi(1, s, c), psi(1, partner, c), -hop_sign * pr)
        else:
            re = signed_sum(psi(0, s, c), psi(1, partner, c), hop_sign * pi)
            im = signed_sum(psi(1, s, c), psi(0, partner, c), -hop_sign * pi)
        row.append((re, im))
    return row


def color_product(link, row):
    out = []
    for r in range(3):
        re = im = None
        for c in range(3):
            lr, li = link(0, r, c), link(1, r, c)
            hr, hi = row[c]
            tr = lr * hr - li * hi
            ti = lr * hi + li * hr
            re = tr if re is None else re + tr
            im = ti if im is None else im + ti
        out.append((re, im))
    return out


def add_rebuilt(total, row, direction, hop_sign, s):
    low = GAMMA_PERM[direction].index(s)
    pr, pi = GAMMA_PHASE[direction][low]
    for c in range(3):
        kr, ki = row[c]
        total[0, s, c] = total[0, s, c] + kr
        total[1, s, c] = total[1, s, c] + ki
        if pi == 0:
            total[0, low, c] = signed_sum(total[0, low, c], kr, -hop_sign * pr)
            total[1, low, c] = signed_sum(total[1, low, c], ki, -hop_sign * pr)
        else:
            total[0, low, c] = signed_sum(total[0, low, c], ki, hop_sign * pi)
            total[1, low, c] = signed_sum(total[1, low, c], kr, -hop_sign * pi)


def packed(pair):
    return jnp.concatenate(pair, 0).astype(jnp.bfloat16)


def widened(tile):
    wide = tile.astype(jnp.float32)
    return wide[:8], wide[8:]


def shift_sites(tile, direction, steps):
    lane = lax.broadcasted_iota(jnp.int32, (8, LANES), 1)
    if direction == 0:
        column = lane % NX
        if steps > 0:
            return jnp.where(
                column == NX - 1,
                pltpu.roll(tile, NX - 1, axis=1),
                pltpu.roll(tile, LANES - 1, axis=1),
            )
        return jnp.where(
            column == 0,
            pltpu.roll(tile, LANES - (NX - 1), axis=1),
            pltpu.roll(tile, 1, axis=1),
        )
    near = pltpu.roll(tile, LANES - NX if steps > 0 else NX, axis=1)
    first_half = lax.broadcasted_iota(jnp.int32, (8, LANES), 0) % 2 == 0
    other = jnp.where(first_half, pltpu.roll(near, 7, axis=0), pltpu.roll(near, 1, axis=0))
    return jnp.where(lane >= LANES - NX if steps > 0 else lane < NX, other, near)


def plane(ri, s, c):
    return (ri * 4 + s) * 3 + c


def link_slot(direction, hop_sign):
    return direction * 2 + (0 if hop_sign > 0 else 1)


def kernel(
    groups, source_hbm, gauge_hbm, out, source, gauge, wide, psi, acc, links, sent, got,
    send_sem, final_sem,
):
    chunks = 2 * groups
    ta, gz = lax.axis_index("ta"), lax.axis_index("gz")
    nt, nz = lax.axis_size("ta"), lax.axis_size("gz")
    above_t = (lax.rem(ta + 1, nt), gz)
    below_t = (lax.rem(ta + nt - 1, nt), gz)
    above_z = (ta, lax.rem(gz + 1, nz))
    below_z = (ta, lax.rem(gz + nz - 1, nz))
    targets = (below_t, above_t, below_z, above_z)

    def landed(ref, semaphore):
        return pltpu.make_async_remote_copy(
            src_ref=ref, dst_ref=ref, send_sem=send_sem.at[0], recv_sem=semaphore,
            device_id=above_t, device_id_type=MESH,
        )

    def load_link(direction, hop_sign):
        slot = link_slot(direction, hop_sign)
        return lambda ri, r, c: links[slot, ri * 9 + r * 3 + c]

    def add_halo(total, step, slot, q, s, halo):
        direction, hop_sign = HALOS[halo]
        row = [widened(got[step, q, slot, 16 * c : 16 * c + 16]) for c in range(3)]
        if hop_sign > 0:
            row = color_product(load_link(direction, 1), row)
        add_rebuilt(total, row, direction, hop_sign, s)

    def rows_of(ri, s, c, g):
        return pl.ds(((ri * 3 + c) * groups + g) * 32 + s, 8, stride=4)

    def load_psi(step, g):
        return lambda ri, s, c: psi[step, g, plane(ri, s, c)]

    def plane_hops(step):
        def body(g, carry):
            at = load_psi(step, g)
            total = {key: at(*key) for key in COMPONENTS}
            for direction in (0, 1):
                for hop_sign in (1, -1):
                    for s in range(2):
                        row = [
                            tuple(shift_sites(v, direction, hop_sign) for v in pair)
                            for pair in project_row(at, direction, hop_sign, s)
                        ]
                        row = color_product(load_link(direction, hop_sign), row)
                        add_rebuilt(total, row, direction, hop_sign, s)
            for key, tile in total.items():
                acc[g, plane(*key)] = tile
            return carry

        lax.fori_loop(0, groups, body, 0)

    def first_application(load_sem, stage_sem, ready):
        def block_loads(g):
            rows = groups * 4
            return [
                pltpu.make_async_copy(
                    source_hbm.at[pl.ds(block * rows + 4 * g, 4)],
                    source.at[pl.ds(block * rows + 4 * g, 4)],
                    load_sem.at[g],
                )
                for block in range(6)
            ]

        def source_group(g):
            return pltpu.make_async_copy(
                source_hbm.at[pl.ds(0, 24)], source.at[pl.ds(0, 24)], load_sem.at[g]
            )

        far_gauge = pltpu.make_async_copy(
            gauge_hbm.at[pl.ds(18, 18)], gauge.at[pl.ds(18, 18)], load_sem.at[groups]
        )
        near_gauge = pltpu.make_async_copy(
            gauge_hbm.at[pl.ds(0, 18)], gauge.at[pl.ds(0, 18)], load_sem.at[groups + 1]
        )
        far_gauge.start()
        for g in range(groups):
            for load in block_loads(g):
                load.start()
        near_gauge.start()

        barrier = pltpu.get_barrier_semaphore()

        def signal_when(condition, semaphore, target):
            @pl.when(condition)
            def _():
                pl.semaphore_signal(semaphore, inc=1, device_id=target, device_id_type=MESH)

        def wait_for(semaphore, *conditions):
            count = sum(c.astype(jnp.int32) for c in conditions)

            @pl.when(count > 0)
            def _():
                pl.semaphore_wait(semaphore, count)

        first_t, last_t, first_z, last_z = ta == 0, ta == nt - 1, gz == 0, gz == nz - 1
        stands_back = (lax.rem(ta, 2) == 1) & (ta > 1) & ~last_t
        even, odd = lax.rem(ta, 2) == 0, lax.rem(ta, 2) == 1
        met_below_t, met_above_t = (ta > 0) & (ta != nt // 2), last_t | (ta == nt // 2 - 1)
        met_below_z, met_above_z = ~first_z, last_z
        signal_when(~met_above_t, barrier, above_t)
        signal_when(~met_below_t, barrier, below_t)
        signal_when(~met_above_z, barrier, above_z)
        signal_when(~met_below_z, barrier, below_z)
        wait_for(barrier, met_below_t, met_above_t, met_below_z, met_above_z)
        signal_when(met_above_z, ready.at[2], above_z)
        signal_when(met_below_z, ready.at[1], below_z)
        signal_when(met_below_t, ready.at[0], below_t)
        signal_when(met_above_t, ready.at[0], above_t)

        upper = (2 * gz) // nz

        def is_late(halo):
            there = (2 * lax.rem(gz + (nz - 1 if halo == 2 else 1), nz)) // nz
            return there if halo == 2 else 1 - there

        def start_halo(step, halo, q):
            if step == 1:
                slot, semaphore = halo, final_sem.at[jnp.maximum(q - (chunks - 3), 0)]
            elif halo < 2:
                slot, semaphore = halo, stage_sem.at[0, q]
            else:
                late = is_late(halo)
                slot, semaphore = 2 + late, stage_sem.at[late, q]
            pltpu.make_async_remote_copy(
                src_ref=sent.at[step, halo, q],
                dst_ref=got.at[step, q, slot],
                send_sem=send_sem.at[0],
                recv_sem=semaphore,
                device_id=targets[halo],
                device_id_type=MESH,
            ).start()

        def start_all(*halos, step=0):
            def one(q, carry):
                for condition, halo in halos:
                    @pl.when(condition)
                    def _():
                        start_halo(step, halo, q)
                return carry

            lax.fori_loop(0, chunks, one, 0)

        def put_halo(step, halo, q, s, at):
            direction, hop_sign = HALOS[halo]
            row = project_row(at, direction, hop_sign, s)
            if hop_sign < 0:
                row = color_product(load_link(direction, -1), row)
            for c in range(3):
                sent[step, halo, q, 16 * c : 16 * c + 16] = packed(row[c])

        first_half = lax.broadcasted_iota(jnp.int32, (8, LANES), 0) % 2 == 0

        def spread(rows, ri, scale):
            return scale * jnp.where(
                first_half,
                jnp.broadcast_to(rows[ri : ri + 1], (8, LANES)),
                jnp.broadcast_to(rows[2 + ri : 3 + ri], (8, LANES)),
            )

        def put_links(*directions):
            for direction in directions:
                scale = jnp.float32(-HOPPING)
                if direction == 3:
                    scale = jnp.where(last_t, HOPPING, -HOPPING).astype(jnp.float32)
                for r in range(3):
                    for c in range(3):
                        rows = gauge[direction * 9 + r * 3 + c].astype(jnp.float32)
                        for ri in range(2):
                            tile = spread(rows, ri, scale)
                            links[link_slot(direction, 1), ri * 9 + r * 3 + c] = tile
                            if direction < 2:
                                tile = shift_sites(tile, direction, -1)
                            links[link_slot(direction, -1), ri * 9 + c * 3 + r] = tile if ri == 0 else -tile

        def start_when(condition, halo, g):
            @pl.when(condition)
            def _():
                for s in range(2):
                    start_halo(0, halo, 2 * g + s)

        far_gauge.wait()
        put_links(3, 2)
        for g in range(groups):
            source_group(g).wait()
            for block in range(6):
                for p in range(4):
                    at = (block * groups + g) * 4 + p
                    wide[8 * at : 8 * at + 8] = source[at].astype(jnp.float32)
            tiles = {(ri, s, c): wide[rows_of(ri, s, c, g)] for ri, s, c in COMPONENTS}
            for halo in range(4):
                for s in range(2):
                    put_halo(0, halo, 2 * g + s, s, lambda *k: tiles[k])
            for k, tile in tiles.items():
                psi[0, g, plane(*k)] = tile
            start_when(last_z & ~stands_back, 3, g)
            start_when(met_below_z & ~last_z, 2, g)
            start_when(met_below_t, 0, g)
            start_when(met_above_t, 1, g)
        start_all((last_z, 2))
        wait_for(ready.at[1], ~met_above_z)
        start_all((~met_above_z, 3))
        wait_for(ready.at[0], ~met_above_t, ~met_below_t)
        start_all((~met_above_t, 1), (~met_below_t, 0))
        start_all((last_z & stands_back, 3))

        near_gauge.wait()
        put_links(0, 1)

        plane_hops(0)
        wait_for(ready.at[2], first_z)
        start_all((first_z, 2))

        held = last_z & (ta == 1)

        def stages(near, far):
            def early(g, carry):
                for s in range(2):
                    q = 2 * g + s
                    total = {k: acc[g, plane(*k)] for k in COMPONENTS if k[1] in (s, s + 2)}
                    landed(got.at[0, q, pl.ds(0, 3)], stage_sem.at[0, q]).wait_recv()
                    add_halo(total, 0, 0, q, s, 0)
                    add_halo(total, 0, 1, q, s, 1)
                    add_halo(total, 0, 2, q, s, near)
                    put_halo(1, near, q, s, lambda *k: total[k])
                    if near == 3:
                        @pl.when(~held)
                        def _():
                            start_halo(1, near, q)
                    else:
                        start_halo(1, near, q)
                    for k, tile in total.items():
                        acc[g, plane(*k)] = tile
                return carry

            def late(g, carry):
                for s in range(2):
                    q = 2 * g + s
                    total = {k: acc[g, plane(*k)] for k in COMPONENTS if k[1] in (s, s + 2)}
                    landed(got.at[0, q, 3], stage_sem.at[1, q]).wait_recv()
                    add_halo(total, 0, 3, q, s, far)
                    for s2 in (s, s + 2):
                        for c in range(3):
                            total[0, s2, c], total[1, s2, c] = widened(
                                packed([total[0, s2, c], total[1, s2, c]])
                            )
                    for halo in (0, 1, far):
                        put_halo(1, halo, q, s, lambda *k: total[k])
                    for halo in (0, 1, far):
                        start_halo(1, halo, q)
                    for k, tile in total.items():
                        psi[1, g, plane(*k)] = tile
                return carry

            lax.fori_loop(0, groups, early, 0)
            if near == 3:
                start_all((held, 3), step=1)
            lax.fori_loop(0, groups, late, 0)

        @pl.when(upper == 0)
        def _():
            stages(2, 3)

        @pl.when(upper == 1)
        def _():
            stages(3, 2)

    pl.run_scoped(
        first_application,
        pltpu.SemaphoreType.DMA((groups + 2,)),
        pltpu.SemaphoreType.DMA((2, chunks)),
        pltpu.SemaphoreType.REGULAR((3,)),
    )
    plane_hops(1)

    for g in range(groups):
        for s in range(2):
            q = 2 * g + s
            total = {k: acc[g, plane(*k)] for k in COMPONENTS if k[1] in (s, s + 2)}
            if q == 0:
                landed(got.at[1, pl.ds(0, chunks - 2)], final_sem.at[0]).wait_recv()
            elif q > chunks - 3:
                landed(got.at[1, q], final_sem.at[q - (chunks - 3)]).wait_recv()
            for halo in range(4):
                add_halo(total, 1, halo, q, s, halo)
            for (ri, s2, c), tile in total.items():
                wide[rows_of(ri, s2, c, g)] = tile
        for block in range(6):
            for p in range(4):
                at = (block * groups + g) * 4 + p
                out[at] = wide[pl.ds(8 * at, 8)].astype(jnp.bfloat16)
    landed(sent, final_sem.at[0]).wait_send()


def body(source, gauge_field):
    rhs = source.shape[5]
    groups = rhs // 4
    chunks = 2 * groups
    source_rows = source.reshape(2, 4, 3, rhs, 2, LANES).transpose(0, 2, 3, 4, 1, 5)
    source_rows = source_rows.reshape(6 * rhs, 8, LANES)
    gauge_rows = gauge_field.reshape(4, 2, 3, 3, 2, LANES).transpose(0, 2, 3, 4, 1, 5)
    gauge_rows = gauge_rows.reshape(36, 4, LANES)
    rows = pl.pallas_call(
        functools.partial(kernel, groups),
        out_shape=pltpu.VMEM(source_rows.shape, source.dtype),
        in_specs=[pl.BlockSpec(memory_space=pltpu.HBM)] * 2,
        out_specs=pl.BlockSpec(memory_space=pltpu.VMEM),
        scratch_shapes=[
            pltpu.VMEM(source_rows.shape, jnp.bfloat16),
            pltpu.VMEM(gauge_rows.shape, jnp.bfloat16),
            pltpu.VMEM((48 * rhs, LANES), jnp.float32),
            pltpu.VMEM((2, groups, 24, 8, LANES), jnp.float32),
            pltpu.VMEM((groups, 24, 8, LANES), jnp.float32),
            pltpu.VMEM((8, 18, 8, LANES), jnp.float32),
            pltpu.VMEM((2, 4, chunks, 48, LANES), jnp.bfloat16),
            pltpu.VMEM((2, chunks, 4, 48, LANES), jnp.bfloat16),
            pltpu.SemaphoreType.DMA((1,)),
            pltpu.SemaphoreType.DMA((3,)),
        ],
        compiler_params=pltpu.CompilerParams(collective_id=0, has_side_effects=True),
        name="dirac_twice",
    )(source_rows, gauge_rows)
    out = rows.reshape(2, 3, rhs, 2, 4, LANES).transpose(0, 4, 1, 2, 3, 5)
    return out.reshape(source.shape)


def solution(mesh):
    spec = P("ta", "gz", None, None, None, None, None)
    return jax.shard_map(body, mesh=mesh, in_specs=(spec, spec), out_specs=spec, check_vma=False)
```

```python
import functools

import jax
import jax.numpy as jnp
from jax import lax
from jax.experimental import pallas as pl
from jax.experimental.pallas import tpu as pltpu
from jax.sharding import PartitionSpec as P

NX = 16
HOPPING = 0.124
GAMMA_PERM = ((3, 2, 1, 0), (3, 2, 1, 0), (2, 3, 0, 1), (2, 3, 0, 1))
GAMMA_PHASE = (
    ((0, 1), (0, 1), (0, -1), (0, -1)),
    ((-1, 0), (1, 0), (1, 0), (-1, 0)),
    ((0, 1), (0, -1), (0, -1), (0, 1)),
    ((1, 0), (1, 0), (1, 0), (1, 0)),
)
LANES = 128
MESH = pl.DeviceIdType.MESH
COMPONENTS = [(ri, s, c) for ri in range(2) for s in range(4) for c in range(3)]

HALOS = ((3, 1), (3, -1), (2, 1), (2, -1))


def signed_sum(base, term, sign):
    return base + term if sign > 0 else base - term


def project_row(psi, direction, hop_sign, s):
    partner = GAMMA_PERM[direction][s]
    pr, pi = GAMMA_PHASE[direction][s]
    row = []
    for c in range(3):
        if pi == 0:
            re = signed_sum(psi(0, s, c), psi(0, partner, c), -hop_sign * pr)
            im = signed_sum(psi(1, s, c), psi(1, partner, c), -hop_sign * pr)
        else:
            re = signed_sum(psi(0, s, c), psi(1, partner, c), hop_sign * pi)
            im = signed_sum(psi(1, s, c), psi(0, partner, c), -hop_sign * pi)
        row.append((re, im))
    return row


def color_product(link, row):
    out = []
    for r in range(3):
        re = im = None
        for c in range(3):
            lr, li = link(0, r, c), link(1, r, c)
            hr, hi = row[c]
            tr = lr * hr - li * hi
            ti = lr * hi + li * hr
            re = tr if re is None else re + tr
            im = ti if im is None else im + ti
        out.append((re, im))
    return out


def add_rebuilt(total, row, direction, hop_sign, s):
    low = GAMMA_PERM[direction].index(s)
    pr, pi = GAMMA_PHASE[direction][low]
    for c in range(3):
        kr, ki = row[c]
        total[0, s, c] = total[0, s, c] + kr
        total[1, s, c] = total[1, s, c] + ki
        if pi == 0:
            total[0, low, c] = signed_sum(total[0, low, c], kr, -hop_sign * pr)
            total[1, low, c] = signed_sum(total[1, low, c], ki, -hop_sign * pr)
        else:
            total[0, low, c] = signed_sum(total[0, low, c], ki, hop_sign * pi)
            total[1, low, c] = signed_sum(total[1, low, c], kr, -hop_sign * pi)


def packed(pair):
    return jnp.concatenate(pair, 0).astype(jnp.bfloat16)


def widened(tile):
    wide = tile.astype(jnp.float32)
    return wide[:8], wide[8:]


def shift_sites(tile, direction, steps):
    lane = lax.broadcasted_iota(jnp.int32, (8, LANES), 1)
    if direction == 0:
        column = lane % NX
        if steps > 0:
            return jnp.where(
                column == NX - 1,
                pltpu.roll(tile, NX - 1, axis=1),
                pltpu.roll(tile, LANES - 1, axis=1),
            )
        return jnp.where(
            column == 0,
            pltpu.roll(tile, LANES - (NX - 1), axis=1),
            pltpu.roll(tile, 1, axis=1),
        )
    near = pltpu.roll(tile, LANES - NX if steps > 0 else NX, axis=1)
    first_half = lax.broadcasted_iota(jnp.int32, (8, LANES), 0) % 2 == 0
    other = jnp.where(first_half, pltpu.roll(near, 7, axis=0), pltpu.roll(near, 1, axis=0))
    return jnp.where(lane >= LANES - NX if steps > 0 else lane < NX, other, near)


def plane(ri, s, c):
    return (ri * 4 + s) * 3 + c


def link_slot(direction, hop_sign):
    return direction * 2 + (0 if hop_sign > 0 else 1)


def kernel(
    groups, source_hbm, gauge_hbm, out, source, gauge, wide, psi, acc, links, sent, got,
    send_sem, final_sem,
):
    chunks = 2 * groups
    ta, gz = lax.axis_index("ta"), lax.axis_index("gz")
    nt, nz = lax.axis_size("ta"), lax.axis_size("gz")
    above_t = (lax.rem(ta + 1, nt), gz)
    below_t = (lax.rem(ta + nt - 1, nt), gz)
    above_z = (ta, lax.rem(gz + 1, nz))
    below_z = (ta, lax.rem(gz + nz - 1, nz))
    targets = (below_t, above_t, below_z, above_z)

    def landed(ref, semaphore):
        return pltpu.make_async_remote_copy(
            src_ref=ref, dst_ref=ref, send_sem=send_sem.at[0], recv_sem=semaphore,
            device_id=above_t, device_id_type=MESH,
        )

    def load_link(direction, hop_sign):
        slot = link_slot(direction, hop_sign)
        return lambda ri, r, c: links[slot, ri * 9 + r * 3 + c]

    def add_halo(total, step, slot, q, s, halo):
        direction, hop_sign = HALOS[halo]
        row = [widened(got[step, q, slot, 16 * c : 16 * c + 16]) for c in range(3)]
        if hop_sign > 0:
            row = color_product(load_link(direction, 1), row)
        add_rebuilt(total, row, direction, hop_sign, s)

    def rows_of(ri, s, c, g):
        return pl.ds(((ri * 3 + c) * groups + g) * 32 + s, 8, stride=4)

    def load_psi(step, g):
        return lambda ri, s, c: psi[step, g, plane(ri, s, c)]

    def plane_hops(step):
        def body(g, carry):
            at = load_psi(step, g)
            total = {key: at(*key) for key in COMPONENTS}
            for direction in (0, 1):
                for hop_sign in (1, -1):
                    for s in range(2):
                        row = [
                            tuple(shift_sites(v, direction, hop_sign) for v in pair)
                            for pair in project_row(at, direction, hop_sign, s)
                        ]
                        row = color_product(load_link(direction, hop_sign), row)
                        add_rebuilt(total, row, direction, hop_sign, s)
            for key, tile in total.items():
                acc[g, plane(*key)] = tile
            return carry

        lax.fori_loop(0, groups, body, 0)

    def first_application(load_sem, stage_sem, ready):
        def source_group(g):
            piece = pl.ds(4 * g, 4)
            return pltpu.make_async_copy(
                source_hbm.at[:, piece], source.at[:, piece], load_sem.at[g]
            )

        far_gauge = pltpu.make_async_copy(
            gauge_hbm.at[pl.ds(18, 18)], gauge.at[pl.ds(18, 18)], load_sem.at[groups]
        )
        near_gauge = pltpu.make_async_copy(
            gauge_hbm.at[pl.ds(0, 18)], gauge.at[pl.ds(0, 18)], load_sem.at[groups + 1]
        )
        for g in range(groups):
            source_group(g).start()
            if g == 0:
                far_gauge.start()
        near_gauge.start()

        barrier = pltpu.get_barrier_semaphore()

        def signal_when(condition, semaphore, target):
            @pl.when(condition)
            def _():
                pl.semaphore_signal(semaphore, inc=1, device_id=target, device_id_type=MESH)

        def wait_for(semaphore, *conditions):
            count = sum(c.astype(jnp.int32) for c in conditions)

            @pl.when(count > 0)
            def _():
                pl.semaphore_wait(semaphore, count)

        first_t, last_t, first_z, last_z = ta == 0, ta == nt - 1, gz == 0, gz == nz - 1
        stands_back = (lax.rem(ta, 2) == 1) & (ta > 1) & ~last_t
        met_below_t, met_above_t = (ta > 0) & (ta != nt // 2), last_t | (ta == nt // 2 - 1)
        met_below_z, met_above_z = ~first_z, last_z
        signal_when(~met_above_t, barrier, above_t)
        signal_when(~met_below_t, barrier, below_t)
        signal_when(~met_above_z, barrier, above_z)
        signal_when(~met_below_z, barrier, below_z)
        wait_for(barrier, met_below_t, met_above_t, met_below_z, met_above_z)
        signal_when(met_above_z, ready.at[2], above_z)
        signal_when(met_below_z, ready.at[1], below_z)
        signal_when(met_below_t, ready.at[0], below_t)
        signal_when(met_above_t, ready.at[0], above_t)

        upper = (2 * gz) // nz

        def is_late(halo):
            there = (2 * lax.rem(gz + (nz - 1 if halo == 2 else 1), nz)) // nz
            return there if halo == 2 else 1 - there

        def start_halo(step, halo, q):
            if step == 1:
                slot, semaphore = halo, final_sem.at[jnp.maximum(q - (chunks - 3), 0)]
            elif halo < 2:
                slot, semaphore = halo, stage_sem.at[0, q]
            else:
                late = is_late(halo)
                slot, semaphore = 2 + late, stage_sem.at[late, q]
            pltpu.make_async_remote_copy(
                src_ref=sent.at[step, halo, q],
                dst_ref=got.at[step, q, slot],
                send_sem=send_sem.at[0],
                recv_sem=semaphore,
                device_id=targets[halo],
                device_id_type=MESH,
            ).start()

        def start_all(*halos, step=0):
            def one(q, carry):
                for condition, halo in halos:
                    @pl.when(condition)
                    def _():
                        start_halo(step, halo, q)
                return carry

            lax.fori_loop(0, chunks, one, 0)

        def put_halo(step, halo, q, s, at):
            direction, hop_sign = HALOS[halo]
            row = project_row(at, direction, hop_sign, s)
            if hop_sign < 0:
                row = color_product(load_link(direction, -1), row)
            for c in range(3):
                sent[step, halo, q, 16 * c : 16 * c + 16] = packed(row[c])

        first_half = lax.broadcasted_iota(jnp.int32, (8, LANES), 0) % 2 == 0

        def spread(rows, ri, scale):
            return scale * jnp.where(
                first_half,
                jnp.broadcast_to(rows[ri : ri + 1], (8, LANES)),
                jnp.broadcast_to(rows[2 + ri : 3 + ri], (8, LANES)),
            )

        def put_links(*directions):
            for direction in directions:
                scale = jnp.float32(-HOPPING)
                if direction == 3:
                    scale = jnp.where(last_t, HOPPING, -HOPPING).astype(jnp.float32)
                for r in range(3):
                    for c in range(3):
                        rows = gauge[direction * 9 + r * 3 + c].astype(jnp.float32)
                        for ri in range(2):
                            tile = spread(rows, ri, scale)
                            links[link_slot(direction, 1), ri * 9 + r * 3 + c] = tile
                            if direction < 2:
                                tile = shift_sites(tile, direction, -1)
                            links[link_slot(direction, -1), ri * 9 + c * 3 + r] = tile if ri == 0 else -tile

        def start_when(condition, halo, g):
            @pl.when(condition)
            def _():
                for s in range(2):
                    start_halo(0, halo, 2 * g + s)

        for g in range(groups):
            source_group(g).wait()
            for block in range(6):
                for p in range(4):
                    at = (block * groups + g) * 4 + p
                    wide[8 * at : 8 * at + 8] = source[block, 4 * g + p].astype(jnp.float32)
            tiles = {(ri, s, c): wide[rows_of(ri, s, c, g)] for ri, s, c in COMPONENTS}
            if g == 0:
                far_gauge.wait()
                put_links(3, 2)
            for halo in range(4):
                for s in range(2):
                    put_halo(0, halo, 2 * g + s, s, lambda *k: tiles[k])
            for k, tile in tiles.items():
                psi[0, g, plane(*k)] = tile
            start_when(last_z & ~stands_back, 3, g)
            start_when(met_below_z & ~last_z, 2, g)
            start_when(met_below_t, 0, g)
            start_when(met_above_t, 1, g)
        start_all((last_z, 2))
        wait_for(ready.at[1], ~met_above_z)
        start_all((~met_above_z, 3))
        wait_for(ready.at[0], ~met_above_t, ~met_below_t)
        start_all((~met_above_t, 1), (~met_below_t, 0))
        start_all((last_z & stands_back, 3))

        near_gauge.wait()
        put_links(0, 1)

        plane_hops(0)
        wait_for(ready.at[2], first_z)
        start_all((first_z, 2))

        held = last_z & (ta == 1)

        def stages(near, far):
            def early(g, carry):
                for s in range(2):
                    q = 2 * g + s
                    total = {k: acc[g, plane(*k)] for k in COMPONENTS if k[1] in (s, s + 2)}
                    landed(got.at[0, q, pl.ds(0, 3)], stage_sem.at[0, q]).wait_recv()
                    add_halo(total, 0, 0, q, s, 0)
                    add_halo(total, 0, 1, q, s, 1)
                    add_halo(total, 0, 2, q, s, near)
                    put_halo(1, near, q, s, lambda *k: total[k])
                    if near == 3:
                        @pl.when(~held)
                        def _():
                            start_halo(1, near, q)
                    else:
                        start_halo(1, near, q)
                    for k, tile in total.items():
                        acc[g, plane(*k)] = tile
                return carry

            def late(g, carry):
                for s in range(2):
                    q = 2 * g + s
                    total = {k: acc[g, plane(*k)] for k in COMPONENTS if k[1] in (s, s + 2)}
                    landed(got.at[0, q, 3], stage_sem.at[1, q]).wait_recv()
                    add_halo(total, 0, 3, q, s, far)
                    for s2 in (s, s + 2):
                        for c in range(3):
                            total[0, s2, c], total[1, s2, c] = widened(
                                packed([total[0, s2, c], total[1, s2, c]])
                            )
                    for halo in (0, 1, far):
                        put_halo(1, halo, q, s, lambda *k: total[k])
                    for halo in (0, 1, far):
                        start_halo(1, halo, q)
                    for k, tile in total.items():
                        psi[1, g, plane(*k)] = tile
                return carry

            lax.fori_loop(0, groups, early, 0)
            if near == 3:
                start_all((held, 3), step=1)
            lax.fori_loop(0, groups, late, 0)

        @pl.when(upper == 0)
        def _():
            stages(2, 3)

        @pl.when(upper == 1)
        def _():
            stages(3, 2)

    pl.run_scoped(
        first_application,
        pltpu.SemaphoreType.DMA((groups + 2,)),
        pltpu.SemaphoreType.DMA((2, chunks)),
        pltpu.SemaphoreType.REGULAR((3,)),
    )
    plane_hops(1)

    for g in range(groups):
        for s in range(2):
            q = 2 * g + s
            total = {k: acc[g, plane(*k)] for k in COMPONENTS if k[1] in (s, s + 2)}
            if q == 0:
                landed(got.at[1, pl.ds(0, chunks - 2)], final_sem.at[0]).wait_recv()
            elif q > chunks - 3:
                landed(got.at[1, q], final_sem.at[q - (chunks - 3)]).wait_recv()
            for halo in range(4):
                add_halo(total, 1, halo, q, s, halo)
            for (ri, s2, c), tile in total.items():
                wide[rows_of(ri, s2, c, g)] = tile
        for block in range(6):
            for p in range(4):
                at = (block * groups + g) * 4 + p
                out[at] = wide[pl.ds(8 * at, 8)].astype(jnp.bfloat16)
    landed(sent, final_sem.at[0]).wait_send()


def body(source, gauge_field):
    rhs = source.shape[5]
    groups = rhs // 4
    chunks = 2 * groups
    source_rows = source.reshape(2, 4, 3, rhs, 2, LANES).transpose(0, 2, 3, 4, 1, 5)
    source_rows = source_rows.reshape(6 * rhs, 8, LANES)
    gauge_rows = gauge_field.reshape(4, 2, 3, 3, 2, LANES).transpose(0, 2, 3, 4, 1, 5)
    gauge_rows = gauge_rows.reshape(36, 4, LANES)
    rows = pl.pallas_call(
        functools.partial(kernel, groups),
        out_shape=pltpu.VMEM(source_rows.shape, source.dtype),
        in_specs=[pl.BlockSpec(memory_space=pltpu.HBM)] * 2,
        out_specs=pl.BlockSpec(memory_space=pltpu.VMEM),
        scratch_shapes=[
            pltpu.VMEM((6, rhs, 8, LANES), jnp.bfloat16),
            pltpu.VMEM(gauge_rows.shape, jnp.bfloat16),
            pltpu.VMEM((48 * rhs, LANES), jnp.float32),
            pltpu.VMEM((2, groups, 24, 8, LANES), jnp.float32),
            pltpu.VMEM((groups, 24, 8, LANES), jnp.float32),
            pltpu.VMEM((8, 18, 8, LANES), jnp.float32),
            pltpu.VMEM((2, 4, chunks, 48, LANES), jnp.bfloat16),
            pltpu.VMEM((2, chunks, 4, 48, LANES), jnp.bfloat16),
            pltpu.SemaphoreType.DMA((1,)),
            pltpu.SemaphoreType.DMA((3,)),
        ],
        compiler_params=pltpu.CompilerParams(collective_id=0, has_side_effects=True),
        name="dirac_twice",
    )(source_rows.reshape(6, rhs, 8, LANES), gauge_rows)
    out = rows.reshape(2, 3, rhs, 2, 4, LANES).transpose(0, 4, 1, 2, 3, 5)
    return out.reshape(source.shape)


def solution(mesh):
    spec = P("ta", "gz", None, None, None, None, None)
    return jax.shard_map(body, mesh=mesh, in_specs=(spec, spec), out_specs=spec, check_vma=False)
```

```python
import functools

import jax
import jax.numpy as jnp
from jax import lax
from jax.experimental import pallas as pl
from jax.experimental.pallas import tpu as pltpu
from jax.sharding import PartitionSpec as P

NX = 16
HOPPING = 0.124
GAMMA_PERM = ((3, 2, 1, 0), (3, 2, 1, 0), (2, 3, 0, 1), (2, 3, 0, 1))
GAMMA_PHASE = (
    ((0, 1), (0, 1), (0, -1), (0, -1)),
    ((-1, 0), (1, 0), (1, 0), (-1, 0)),
    ((0, 1), (0, -1), (0, -1), (0, 1)),
    ((1, 0), (1, 0), (1, 0), (1, 0)),
)
LANES = 128
MESH = pl.DeviceIdType.MESH
COMPONENTS = [(ri, s, c) for ri in range(2) for s in range(4) for c in range(3)]

HALOS = ((3, 1), (3, -1), (2, 1), (2, -1))


def signed_sum(base, term, sign):
    return base + term if sign > 0 else base - term


def project_row(psi, direction, hop_sign, s):
    partner = GAMMA_PERM[direction][s]
    pr, pi = GAMMA_PHASE[direction][s]
    row = []
    for c in range(3):
        if pi == 0:
            re = signed_sum(psi(0, s, c), psi(0, partner, c), -hop_sign * pr)
            im = signed_sum(psi(1, s, c), psi(1, partner, c), -hop_sign * pr)
        else:
            re = signed_sum(psi(0, s, c), psi(1, partner, c), hop_sign * pi)
            im = signed_sum(psi(1, s, c), psi(0, partner, c), -hop_sign * pi)
        row.append((re, im))
    return row


def color_product(link, row):
    out = []
    for r in range(3):
        re = im = None
        for c in range(3):
            lr, li = link(0, r, c), link(1, r, c)
            hr, hi = row[c]
            tr = lr * hr - li * hi
            ti = lr * hi + li * hr
            re = tr if re is None else re + tr
            im = ti if im is None else im + ti
        out.append((re, im))
    return out


def add_rebuilt(total, row, direction, hop_sign, s):
    low = GAMMA_PERM[direction].index(s)
    pr, pi = GAMMA_PHASE[direction][low]
    for c in range(3):
        kr, ki = row[c]
        total[0, s, c] = total[0, s, c] + kr
        total[1, s, c] = total[1, s, c] + ki
        if pi == 0:
            total[0, low, c] = signed_sum(total[0, low, c], kr, -hop_sign * pr)
            total[1, low, c] = signed_sum(total[1, low, c], ki, -hop_sign * pr)
        else:
            total[0, low, c] = signed_sum(total[0, low, c], ki, hop_sign * pi)
            total[1, low, c] = signed_sum(total[1, low, c], kr, -hop_sign * pi)


def packed(pair):
    return jnp.concatenate(pair, 0).astype(jnp.bfloat16)


def widened(tile):
    wide = tile.astype(jnp.float32)
    return wide[:8], wide[8:]


def shift_sites(tile, direction, steps):
    lane = lax.broadcasted_iota(jnp.int32, (8, LANES), 1)
    if direction == 0:
        column = lane % NX
        if steps > 0:
            return jnp.where(
                column == NX - 1,
                pltpu.roll(tile, NX - 1, axis=1),
                pltpu.roll(tile, LANES - 1, axis=1),
            )
        return jnp.where(
            column == 0,
            pltpu.roll(tile, LANES - (NX - 1), axis=1),
            pltpu.roll(tile, 1, axis=1),
        )
    near = pltpu.roll(tile, LANES - NX if steps > 0 else NX, axis=1)
    first_half = lax.broadcasted_iota(jnp.int32, (8, LANES), 0) % 2 == 0
    other = jnp.where(first_half, pltpu.roll(near, 7, axis=0), pltpu.roll(near, 1, axis=0))
    return jnp.where(lane >= LANES - NX if steps > 0 else lane < NX, other, near)


def plane(ri, s, c):
    return (ri * 4 + s) * 3 + c


def link_slot(direction, hop_sign):
    return direction * 2 + (0 if hop_sign > 0 else 1)


def apply_twice(
    groups, source_hbm, gauge_hbm, out, source, gauge, wide, psi, acc, links, sent, got,
    send_sem, final_sem,
):
    chunks = 2 * groups
    ta, gz = lax.axis_index("ta"), lax.axis_index("gz")
    nt, nz = lax.axis_size("ta"), lax.axis_size("gz")
    above_t = (lax.rem(ta + 1, nt), gz)
    below_t = (lax.rem(ta + nt - 1, nt), gz)
    above_z = (ta, lax.rem(gz + 1, nz))
    below_z = (ta, lax.rem(gz + nz - 1, nz))
    targets = (below_t, above_t, below_z, above_z)

    def landed(ref, semaphore):
        return pltpu.make_async_remote_copy(
            src_ref=ref, dst_ref=ref, send_sem=send_sem.at[0], recv_sem=semaphore,
            device_id=above_t, device_id_type=MESH,
        )

    def load_link(direction, hop_sign):
        slot = link_slot(direction, hop_sign)
        return lambda ri, r, c: links[slot, ri * 9 + r * 3 + c]

    def add_halo(total, step, slot, q, s, halo):
        direction, hop_sign = HALOS[halo]
        row = [widened(got[step, q, slot, 16 * c : 16 * c + 16]) for c in range(3)]
        if hop_sign > 0:
            row = color_product(load_link(direction, 1), row)
        add_rebuilt(total, row, direction, hop_sign, s)

    def rows_of(ri, s, c, g):
        return pl.ds(((ri * 3 + c) * groups + g) * 32 + s, 8, stride=4)

    def load_psi(step, g):
        return lambda ri, s, c: psi[step, g, plane(ri, s, c)]

    def plane_hops(step):
        def body(g, carry):
            at = load_psi(step, g)
            total = {key: at(*key) for key in COMPONENTS}
            for direction in (0, 1):
                for hop_sign in (1, -1):
                    for s in range(2):
                        row = [
                            tuple(shift_sites(v, direction, hop_sign) for v in pair)
                            for pair in project_row(at, direction, hop_sign, s)
                        ]
                        row = color_product(load_link(direction, hop_sign), row)
                        add_rebuilt(total, row, direction, hop_sign, s)
            for key, tile in total.items():
                acc[g, plane(*key)] = tile
            return carry

        lax.fori_loop(0, groups, body, 0)

    def first_application(load_sem, stage_sem, ready):
        def source_group(g):
            piece = pl.ds(4 * g, 4)
            return pltpu.make_async_copy(
                source_hbm.at[:, piece], source.at[:, piece], load_sem.at[g]
            )

        far_gauge = pltpu.make_async_copy(
            gauge_hbm.at[pl.ds(18, 18)], gauge.at[pl.ds(18, 18)], load_sem.at[groups]
        )
        near_gauge = pltpu.make_async_copy(
            gauge_hbm.at[pl.ds(0, 18)], gauge.at[pl.ds(0, 18)], load_sem.at[groups + 1]
        )
        for g in range(groups):
            source_group(g).start()
            if g == 0:
                far_gauge.start()
        near_gauge.start()

        barrier = pltpu.get_barrier_semaphore()

        def signal_when(condition, semaphore, target):
            @pl.when(condition)
            def _():
                pl.semaphore_signal(semaphore, inc=1, device_id=target, device_id_type=MESH)

        def wait_for(semaphore, *conditions):
            count = sum(c.astype(jnp.int32) for c in conditions)

            @pl.when(count > 0)
            def _():
                pl.semaphore_wait(semaphore, count)

        first_t, last_t, first_z, last_z = ta == 0, ta == nt - 1, gz == 0, gz == nz - 1
        stands_back = (lax.rem(ta, 2) == 1) & (ta > 1) & ~last_t
        met_below_t = (ta > 0) & (ta != nt // 2) & ~last_t
        met_above_t = last_t | (ta == nt // 2 - 1) | (ta == nt - 2)
        met_below_z, met_above_z = ~first_z, last_z
        signal_when(~met_above_t, barrier, above_t)
        signal_when(~met_below_t, barrier, below_t)
        signal_when(~met_above_z, barrier, above_z)
        signal_when(~met_below_z, barrier, below_z)
        wait_for(barrier, met_below_t, met_above_t, met_below_z, met_above_z)
        signal_when(met_above_z, ready.at[2], above_z)
        signal_when(met_below_z, ready.at[1], below_z)
        signal_when(met_below_t, ready.at[0], below_t)
        signal_when(met_above_t, ready.at[0], above_t)

        upper = (2 * gz) // nz

        def is_late(halo):
            there = (2 * lax.rem(gz + (nz - 1 if halo == 2 else 1), nz)) // nz
            return there if halo == 2 else 1 - there

        def start_halo(step, halo, q):
            if step == 1:
                slot, semaphore = halo, final_sem.at[jnp.maximum(q - (chunks - 3), 0)]
            elif halo < 2:
                slot, semaphore = halo, stage_sem.at[0, q]
            else:
                late = is_late(halo)
                slot, semaphore = 2 + late, stage_sem.at[late, q]
            pltpu.make_async_remote_copy(
                src_ref=sent.at[step, halo, q],
                dst_ref=got.at[step, q, slot],
                send_sem=send_sem.at[0],
                recv_sem=semaphore,
                device_id=targets[halo],
                device_id_type=MESH,
            ).start()

        def start_all(*halos, step=0):
            def one(q, carry):
                for condition, halo in halos:
                    @pl.when(condition)
                    def _():
                        start_halo(step, halo, q)
                return carry

            lax.fori_loop(0, chunks, one, 0)

        def put_halo(step, halo, q, s, at):
            direction, hop_sign = HALOS[halo]
            row = project_row(at, direction, hop_sign, s)
            if hop_sign < 0:
                row = color_product(load_link(direction, -1), row)
            for c in range(3):
                sent[step, halo, q, 16 * c : 16 * c + 16] = packed(row[c])

        first_half = lax.broadcasted_iota(jnp.int32, (8, LANES), 0) % 2 == 0

        def spread(rows, ri, scale):
            return scale * jnp.where(
                first_half,
                jnp.broadcast_to(rows[ri : ri + 1], (8, LANES)),
                jnp.broadcast_to(rows[2 + ri : 3 + ri], (8, LANES)),
            )

        def put_links(*directions):
            for direction in directions:
                scale = jnp.float32(-HOPPING)
                if direction == 3:
                    scale = jnp.where(last_t, HOPPING, -HOPPING).astype(jnp.float32)
                for r in range(3):
                    for c in range(3):
                        rows = gauge[direction * 9 + r * 3 + c].astype(jnp.float32)
                        for ri in range(2):
                            tile = spread(rows, ri, scale)
                            links[link_slot(direction, 1), ri * 9 + r * 3 + c] = tile
                            if direction < 2:
                                tile = shift_sites(tile, direction, -1)
                            links[link_slot(direction, -1), ri * 9 + c * 3 + r] = tile if ri == 0 else -tile

        def start_when(condition, halo, g):
            @pl.when(condition)
            def _():
                for s in range(2):
                    start_halo(0, halo, 2 * g + s)

        for g in range(groups):
            source_group(g).wait()
            for block in range(6):
                for p in range(4):
                    at = (block * groups + g) * 4 + p
                    wide[8 * at : 8 * at + 8] = source[block, 4 * g + p].astype(jnp.float32)
            tiles = {(ri, s, c): wide[rows_of(ri, s, c, g)] for ri, s, c in COMPONENTS}
            if g == 0:
                far_gauge.wait()
                put_links(3, 2)
            for halo in range(4):
                for s in range(2):
                    put_halo(0, halo, 2 * g + s, s, lambda *k: tiles[k])
            for k, tile in tiles.items():
                psi[0, g, plane(*k)] = tile
            start_when(last_z & ~stands_back, 3, g)
            start_when(met_below_z & ~last_z, 2, g)
            start_when(met_below_t, 0, g)
            start_when(met_above_t, 1, g)
        start_all((last_z, 2))
        wait_for(ready.at[1], ~met_above_z)
        start_all((~met_above_z, 3))
        wait_for(ready.at[0], ~met_above_t, ~met_below_t)
        start_all((~met_above_t, 1), (~met_below_t, 0))
        start_all((last_z & stands_back, 3))

        near_gauge.wait()
        put_links(0, 1)

        plane_hops(0)
        wait_for(ready.at[2], first_z)
        start_all((first_z, 2))

        held = last_z & (ta == 1)

        def stages(near, far):
            def early(g, carry):
                for s in range(2):
                    q = 2 * g + s
                    total = {k: acc[g, plane(*k)] for k in COMPONENTS if k[1] in (s, s + 2)}
                    landed(got.at[0, q, pl.ds(0, 3)], stage_sem.at[0, q]).wait_recv()
                    add_halo(total, 0, 0, q, s, 0)
                    add_halo(total, 0, 1, q, s, 1)
                    add_halo(total, 0, 2, q, s, near)
                    put_halo(1, near, q, s, lambda *k: total[k])
                    if near == 3:
                        @pl.when(~held)
                        def _():
                            start_halo(1, near, q)
                    else:
                        start_halo(1, near, q)
                    for k, tile in total.items():
                        acc[g, plane(*k)] = tile
                return carry

            def late(g, carry):
                for s in range(2):
                    q = 2 * g + s
                    total = {k: acc[g, plane(*k)] for k in COMPONENTS if k[1] in (s, s + 2)}
                    landed(got.at[0, q, 3], stage_sem.at[1, q]).wait_recv()
                    add_halo(total, 0, 3, q, s, far)
                    for s2 in (s, s + 2):
                        for c in range(3):
                            total[0, s2, c], total[1, s2, c] = widened(
                                packed([total[0, s2, c], total[1, s2, c]])
                            )
                    for halo in (0, 1, far):
                        put_halo(1, halo, q, s, lambda *k: total[k])
                    for halo in (0, 1, far):
                        start_halo(1, halo, q)
                    for k, tile in total.items():
                        psi[1, g, plane(*k)] = tile
                return carry

            lax.fori_loop(0, groups, early, 0)
            if near == 3:
                start_all((held, 3), step=1)
            lax.fori_loop(0, groups, late, 0)

        @pl.when(upper == 0)
        def _():
            stages(2, 3)

        @pl.when(upper == 1)
        def _():
            stages(3, 2)

    pl.run_scoped(
        first_application,
        pltpu.SemaphoreType.DMA((groups + 2,)),
        pltpu.SemaphoreType.DMA((2, chunks)),
        pltpu.SemaphoreType.REGULAR((3,)),
    )
    plane_hops(1)

    for g in range(groups):
        for s in range(2):
            q = 2 * g + s
            total = {k: acc[g, plane(*k)] for k in COMPONENTS if k[1] in (s, s + 2)}
            if q == 0:
                landed(got.at[1, pl.ds(0, chunks - 2)], final_sem.at[0]).wait_recv()
            elif q > chunks - 3:
                landed(got.at[1, q], final_sem.at[q - (chunks - 3)]).wait_recv()
            for halo in range(4):
                add_halo(total, 1, halo, q, s, halo)
            for (ri, s2, c), tile in total.items():
                wide[rows_of(ri, s2, c, g)] = tile
        for block in range(6):
            for p in range(4):
                at = (block * groups + g) * 4 + p
                out[at] = wide[pl.ds(8 * at, 8)].astype(jnp.bfloat16)
    landed(sent, final_sem.at[0]).wait_send()


def kernel(groups, *refs):
    pl.run_scoped(
        functools.partial(apply_twice, groups, *refs),
        pltpu.SemaphoreType.DMA((1,)),
        pltpu.SemaphoreType.DMA((3,)),
    )


def body(source, gauge_field):
    rhs = source.shape[5]
    groups = rhs // 4
    chunks = 2 * groups
    source_rows = source.reshape(2, 4, 3, rhs, 2, LANES).transpose(0, 2, 3, 4, 1, 5)
    source_rows = source_rows.reshape(6 * rhs, 8, LANES)
    gauge_rows = gauge_field.reshape(4, 2, 3, 3, 2, LANES).transpose(0, 2, 3, 4, 1, 5)
    gauge_rows = gauge_rows.reshape(36, 4, LANES)
    rows = pl.pallas_call(
        functools.partial(kernel, groups),
        out_shape=pltpu.VMEM(source_rows.shape, source.dtype),
        in_specs=[pl.BlockSpec(memory_space=pltpu.HBM)] * 2,
        out_specs=pl.BlockSpec(memory_space=pltpu.VMEM),
        scratch_shapes=[
            pltpu.VMEM((6, rhs, 8, LANES), jnp.bfloat16),
            pltpu.VMEM(gauge_rows.shape, jnp.bfloat16),
            pltpu.VMEM((48 * rhs, LANES), jnp.float32),
            pltpu.VMEM((2, groups, 24, 8, LANES), jnp.float32),
            pltpu.VMEM((groups, 24, 8, LANES), jnp.float32),
            pltpu.VMEM((8, 18, 8, LANES), jnp.float32),
            pltpu.VMEM((2, 4, chunks, 48, LANES), jnp.bfloat16),
            pltpu.VMEM((2, chunks, 4, 48, LANES), jnp.bfloat16),
        ],
        compiler_params=pltpu.CompilerParams(collective_id=0, has_side_effects=True),
        name="dirac_twice",
    )(source_rows.reshape(6, rhs, 8, LANES), gauge_rows)
    out = rows.reshape(2, 3, rhs, 2, 4, LANES).transpose(0, 4, 1, 2, 3, 5)
    return out.reshape(source.shape)


def solution(mesh):
    spec = P("ta", "gz", None, None, None, None, None)
    return jax.shard_map(body, mesh=mesh, in_specs=(spec, spec), out_specs=spec, check_vma=False)
```

```python
import functools

import jax
import jax.numpy as jnp
from jax import lax
from jax.experimental import pallas as pl
from jax.experimental.pallas import tpu as pltpu
from jax.sharding import PartitionSpec as P

NX = 16
HOPPING = 0.124
GAMMA_PERM = ((3, 2, 1, 0), (3, 2, 1, 0), (2, 3, 0, 1), (2, 3, 0, 1))
GAMMA_PHASE = (
    ((0, 1), (0, 1), (0, -1), (0, -1)),
    ((-1, 0), (1, 0), (1, 0), (-1, 0)),
    ((0, 1), (0, -1), (0, -1), (0, 1)),
    ((1, 0), (1, 0), (1, 0), (1, 0)),
)
LANES = 128
MESH = pl.DeviceIdType.MESH
COMPONENTS = [(ri, s, c) for ri in range(2) for s in range(4) for c in range(3)]

HALOS = ((3, 1), (3, -1), (2, 1), (2, -1))


def signed_sum(base, term, sign):
    return base + term if sign > 0 else base - term


def project_row(psi, direction, hop_sign, s):
    partner = GAMMA_PERM[direction][s]
    pr, pi = GAMMA_PHASE[direction][s]
    row = []
    for c in range(3):
        if pi == 0:
            re = signed_sum(psi(0, s, c), psi(0, partner, c), -hop_sign * pr)
            im = signed_sum(psi(1, s, c), psi(1, partner, c), -hop_sign * pr)
        else:
            re = signed_sum(psi(0, s, c), psi(1, partner, c), hop_sign * pi)
            im = signed_sum(psi(1, s, c), psi(0, partner, c), -hop_sign * pi)
        row.append((re, im))
    return row


def color_product(link, row):
    out = []
    for r in range(3):
        re = im = None
        for c in range(3):
            lr, li = link(0, r, c), link(1, r, c)
            hr, hi = row[c]
            tr = lr * hr - li * hi
            ti = lr * hi + li * hr
            re = tr if re is None else re + tr
            im = ti if im is None else im + ti
        out.append((re, im))
    return out


def add_rebuilt(total, row, direction, hop_sign, s):
    low = GAMMA_PERM[direction].index(s)
    pr, pi = GAMMA_PHASE[direction][low]
    for c in range(3):
        kr, ki = row[c]
        total[0, s, c] = total[0, s, c] + kr
        total[1, s, c] = total[1, s, c] + ki
        if pi == 0:
            total[0, low, c] = signed_sum(total[0, low, c], kr, -hop_sign * pr)
            total[1, low, c] = signed_sum(total[1, low, c], ki, -hop_sign * pr)
        else:
            total[0, low, c] = signed_sum(total[0, low, c], ki, hop_sign * pi)
            total[1, low, c] = signed_sum(total[1, low, c], kr, -hop_sign * pi)


def packed(pair):
    return jnp.concatenate(pair, 0).astype(jnp.bfloat16)


def widened(tile):
    wide = tile.astype(jnp.float32)
    return wide[:8], wide[8:]


def shift_sites(tile, direction, steps):
    lane = lax.broadcasted_iota(jnp.int32, (8, LANES), 1)
    if direction == 0:
        column = lane % NX
        if steps > 0:
            return jnp.where(
                column == NX - 1,
                pltpu.roll(tile, NX - 1, axis=1),
                pltpu.roll(tile, LANES - 1, axis=1),
            )
        return jnp.where(
            column == 0,
            pltpu.roll(tile, LANES - (NX - 1), axis=1),
            pltpu.roll(tile, 1, axis=1),
        )
    near = pltpu.roll(tile, LANES - NX if steps > 0 else NX, axis=1)
    first_half = lax.broadcasted_iota(jnp.int32, (8, LANES), 0) % 2 == 0
    other = jnp.where(first_half, pltpu.roll(near, 7, axis=0), pltpu.roll(near, 1, axis=0))
    return jnp.where(lane >= LANES - NX if steps > 0 else lane < NX, other, near)


def plane(ri, s, c):
    return (ri * 4 + s) * 3 + c


def link_slot(direction, hop_sign):
    return direction * 2 + (0 if hop_sign > 0 else 1)


def apply_twice(
    groups, source_hbm, gauge_hbm, out, source, gauge, wide, psi, acc, links, sent, got,
    send_sem, final_sem,
):
    chunks = 2 * groups
    ta, gz = lax.axis_index("ta"), lax.axis_index("gz")
    nt, nz = lax.axis_size("ta"), lax.axis_size("gz")
    above_t = (lax.rem(ta + 1, nt), gz)
    below_t = (lax.rem(ta + nt - 1, nt), gz)
    above_z = (ta, lax.rem(gz + 1, nz))
    below_z = (ta, lax.rem(gz + nz - 1, nz))
    targets = (below_t, above_t, below_z, above_z)

    def landed(ref, semaphore):
        return pltpu.make_async_remote_copy(
            src_ref=ref, dst_ref=ref, send_sem=send_sem.at[0], recv_sem=semaphore,
            device_id=above_t, device_id_type=MESH,
        )

    def load_link(direction, hop_sign):
        slot = link_slot(direction, hop_sign)
        return lambda ri, r, c: links[slot, ri * 9 + r * 3 + c]

    def add_halo(total, step, slot, q, s, halo):
        direction, hop_sign = HALOS[halo]
        row = [widened(got[step, q, slot, 16 * c : 16 * c + 16]) for c in range(3)]
        if hop_sign > 0:
            row = color_product(load_link(direction, 1), row)
        add_rebuilt(total, row, direction, hop_sign, s)

    def rows_of(ri, s, c, g):
        return pl.ds(((ri * 3 + c) * groups + g) * 32 + s, 8, stride=4)

    def load_psi(step, g):
        return lambda ri, s, c: psi[step, g, plane(ri, s, c)]

    def plane_hops(step):
        def body(g, carry):
            at = load_psi(step, g)
            total = {key: at(*key) for key in COMPONENTS}
            for direction in (0, 1):
                for hop_sign in (1, -1):
                    for s in range(2):
                        row = [
                            tuple(shift_sites(v, direction, hop_sign) for v in pair)
                            for pair in project_row(at, direction, hop_sign, s)
                        ]
                        row = color_product(load_link(direction, hop_sign), row)
                        add_rebuilt(total, row, direction, hop_sign, s)
            for key, tile in total.items():
                acc[g, plane(*key)] = tile
            return carry

        lax.fori_loop(0, groups, body, 0)

    def first_application(load_sem, stage_sem, ready):
        def source_group(g):
            piece = pl.ds(4 * g, 4)
            return pltpu.make_async_copy(
                source_hbm.at[:, piece], source.at[:, piece], load_sem.at[g]
            )

        far_gauge = pltpu.make_async_copy(
            gauge_hbm.at[pl.ds(18, 18)], gauge.at[pl.ds(18, 18)], load_sem.at[groups]
        )
        near_gauge = pltpu.make_async_copy(
            gauge_hbm.at[pl.ds(0, 18)], gauge.at[pl.ds(0, 18)], load_sem.at[groups + 1]
        )
        for g in range(groups):
            source_group(g).start()
            if g == 0:
                far_gauge.start()
        near_gauge.start()

        barrier = pltpu.get_barrier_semaphore()

        def signal_when(condition, semaphore, target):
            @pl.when(condition)
            def _():
                pl.semaphore_signal(semaphore, inc=1, device_id=target, device_id_type=MESH)

        def wait_for(semaphore, *conditions):
            count = sum(c.astype(jnp.int32) for c in conditions)

            @pl.when(count > 0)
            def _():
                pl.semaphore_wait(semaphore, count)

        first_t, last_t, first_z, last_z = ta == 0, ta == nt - 1, gz == 0, gz == nz - 1
        stands_back = (lax.rem(ta, 2) == 1) & (ta > 1) & ~last_t
        met_below_t = (ta > 0) & (ta != nt // 2) & ~last_t
        met_above_t = last_t | (ta == nt // 2 - 1) | (ta == nt - 2)
        met_below_z, met_above_z = ~first_z, last_z
        signal_when(~met_above_t, barrier, above_t)
        signal_when(~met_below_t, barrier, below_t)
        signal_when(~met_above_z, barrier, above_z)
        signal_when(~met_below_z, barrier, below_z)
        wait_for(barrier, met_below_t, met_above_t, met_below_z, met_above_z)
        signal_when(met_above_z, ready.at[2], above_z)
        signal_when(met_below_z, ready.at[1], below_z)
        signal_when(met_below_t, ready.at[0], below_t)
        signal_when(met_above_t, ready.at[0], above_t)

        upper = (2 * gz) // nz

        def is_late(halo):
            there = (2 * lax.rem(gz + (nz - 1 if halo == 2 else 1), nz)) // nz
            return there if halo == 2 else 1 - there

        def start_halo(step, halo, q):
            if step == 1:
                slot, semaphore = halo, final_sem.at[jnp.maximum(q - (chunks - 3), 0)]
            elif halo < 2:
                slot, semaphore = halo, stage_sem.at[0, q]
            else:
                late = is_late(halo)
                slot, semaphore = 2 + late, stage_sem.at[late, q]
            pltpu.make_async_remote_copy(
                src_ref=sent.at[step, halo, q],
                dst_ref=got.at[step, q, slot],
                send_sem=send_sem.at[0],
                recv_sem=semaphore,
                device_id=targets[halo],
                device_id_type=MESH,
            ).start()

        def start_all(*halos, step=0):
            def one(q, carry):
                for condition, halo in halos:
                    @pl.when(condition)
                    def _():
                        start_halo(step, halo, q)
                return carry

            lax.fori_loop(0, chunks, one, 0)

        def put_halo(step, halo, q, s, at):
            direction, hop_sign = HALOS[halo]
            row = project_row(at, direction, hop_sign, s)
            if hop_sign < 0:
                row = color_product(load_link(direction, -1), row)
            for c in range(3):
                sent[step, halo, q, 16 * c : 16 * c + 16] = packed(row[c])

        first_half = lax.broadcasted_iota(jnp.int32, (8, LANES), 0) % 2 == 0

        def spread(rows, ri, scale):
            return scale * jnp.where(
                first_half,
                jnp.broadcast_to(rows[ri : ri + 1], (8, LANES)),
                jnp.broadcast_to(rows[2 + ri : 3 + ri], (8, LANES)),
            )

        def put_links(*directions):
            for direction in directions:
                scale = jnp.float32(-HOPPING)
                if direction == 3:
                    scale = jnp.where(last_t, HOPPING, -HOPPING).astype(jnp.float32)
                for r in range(3):
                    for c in range(3):
                        rows = gauge[direction * 9 + r * 3 + c].astype(jnp.float32)
                        for ri in range(2):
                            tile = spread(rows, ri, scale)
                            links[link_slot(direction, 1), ri * 9 + r * 3 + c] = tile
                            if direction < 2:
                                tile = shift_sites(tile, direction, -1)
                            links[link_slot(direction, -1), ri * 9 + c * 3 + r] = tile if ri == 0 else -tile

        def start_when(condition, halo, g):
            @pl.when(condition)
            def _():
                for s in range(2):
                    start_halo(0, halo, 2 * g + s)

        for g in range(groups):
            source_group(g).wait()
            for block in range(6):
                for p in range(4):
                    at = (block * groups + g) * 4 + p
                    wide[8 * at : 8 * at + 8] = source[block, 4 * g + p].astype(jnp.float32)
            tiles = {(ri, s, c): wide[rows_of(ri, s, c, g)] for ri, s, c in COMPONENTS}
            if g == 0:
                far_gauge.wait()
                put_links(3, 2)
            for halo in range(4):
                for s in range(2):
                    put_halo(0, halo, 2 * g + s, s, lambda *k: tiles[k])
            for k, tile in tiles.items():
                psi[0, g, plane(*k)] = tile
            start_when(met_below_t, 0, g)
            start_when(met_above_t, 1, g)
            start_when(last_z & ~stands_back, 3, g)
            start_when(met_below_z & ~last_z, 2, g)
        start_all((last_z, 2))
        wait_for(ready.at[1], ~met_above_z)
        start_all((~met_above_z, 3))
        wait_for(ready.at[0], ~met_above_t, ~met_below_t)
        start_all((~met_above_t, 1), (~met_below_t, 0))
        start_all((last_z & stands_back, 3))

        near_gauge.wait()
        put_links(0, 1)

        plane_hops(0)
        wait_for(ready.at[2], first_z)
        start_all((first_z, 2))

        held = last_z & (ta == 1)

        def stages(near, far):
            def early(g, carry):
                for s in range(2):
                    q = 2 * g + s
                    total = {k: acc[g, plane(*k)] for k in COMPONENTS if k[1] in (s, s + 2)}
                    landed(got.at[0, q, pl.ds(0, 3)], stage_sem.at[0, q]).wait_recv()
                    add_halo(total, 0, 0, q, s, 0)
                    add_halo(total, 0, 1, q, s, 1)
                    add_halo(total, 0, 2, q, s, near)
                    put_halo(1, near, q, s, lambda *k: total[k])
                    if near == 3:
                        @pl.when(~held)
                        def _():
                            start_halo(1, near, q)
                    else:
                        start_halo(1, near, q)
                    for k, tile in total.items():
                        acc[g, plane(*k)] = tile
                return carry

            def late(g, carry):
                for s in range(2):
                    q = 2 * g + s
                    total = {k: acc[g, plane(*k)] for k in COMPONENTS if k[1] in (s, s + 2)}
                    landed(got.at[0, q, 3], stage_sem.at[1, q]).wait_recv()
                    add_halo(total, 0, 3, q, s, far)
                    for s2 in (s, s + 2):
                        for c in range(3):
                            total[0, s2, c], total[1, s2, c] = widened(
                                packed([total[0, s2, c], total[1, s2, c]])
                            )
                    for halo in (0, 1, far):
                        put_halo(1, halo, q, s, lambda *k: total[k])
                    for halo in (0, 1, far):
                        start_halo(1, halo, q)
                    for k, tile in total.items():
                        psi[1, g, plane(*k)] = tile
                return carry

            lax.fori_loop(0, groups, early, 0)
            if near == 3:
                start_all((held, 3), step=1)
            lax.fori_loop(0, groups, late, 0)

        @pl.when(upper == 0)
        def _():
            stages(2, 3)

        @pl.when(upper == 1)
        def _():
            stages(3, 2)

    pl.run_scoped(
        first_application,
        pltpu.SemaphoreType.DMA((groups + 2,)),
        pltpu.SemaphoreType.DMA((2, chunks)),
        pltpu.SemaphoreType.REGULAR((3,)),
    )
    plane_hops(1)

    for g in range(groups):
        for s in range(2):
            q = 2 * g + s
            total = {k: acc[g, plane(*k)] for k in COMPONENTS if k[1] in (s, s + 2)}
            if q == 0:
                landed(got.at[1, pl.ds(0, chunks - 2)], final_sem.at[0]).wait_recv()
            elif q > chunks - 3:
                landed(got.at[1, q], final_sem.at[q - (chunks - 3)]).wait_recv()
            for halo in range(4):
                add_halo(total, 1, halo, q, s, halo)
            for (ri, s2, c), tile in total.items():
                wide[rows_of(ri, s2, c, g)] = tile
        for block in range(6):
            for p in range(4):
                at = (block * groups + g) * 4 + p
                out[at] = wide[pl.ds(8 * at, 8)].astype(jnp.bfloat16)
    landed(sent, final_sem.at[0]).wait_send()


def kernel(groups, *refs):
    pl.run_scoped(
        functools.partial(apply_twice, groups, *refs),
        pltpu.SemaphoreType.DMA((1,)),
        pltpu.SemaphoreType.DMA((3,)),
    )


def body(source, gauge_field):
    rhs = source.shape[5]
    groups = rhs // 4
    chunks = 2 * groups
    source_rows = source.reshape(2, 4, 3, rhs, 2, LANES).transpose(0, 2, 3, 4, 1, 5)
    source_rows = source_rows.reshape(6 * rhs, 8, LANES)
    gauge_rows = gauge_field.reshape(4, 2, 3, 3, 2, LANES).transpose(0, 2, 3, 4, 1, 5)
    gauge_rows = gauge_rows.reshape(36, 4, LANES)
    rows = pl.pallas_call(
        functools.partial(kernel, groups),
        out_shape=pltpu.VMEM(source_rows.shape, source.dtype),
        in_specs=[pl.BlockSpec(memory_space=pltpu.HBM)] * 2,
        out_specs=pl.BlockSpec(memory_space=pltpu.VMEM),
        scratch_shapes=[
            pltpu.VMEM((6, rhs, 8, LANES), jnp.bfloat16),
            pltpu.VMEM(gauge_rows.shape, jnp.bfloat16),
            pltpu.VMEM((48 * rhs, LANES), jnp.float32),
            pltpu.VMEM((2, groups, 24, 8, LANES), jnp.float32),
            pltpu.VMEM((groups, 24, 8, LANES), jnp.float32),
            pltpu.VMEM((8, 18, 8, LANES), jnp.float32),
            pltpu.VMEM((2, 4, chunks, 48, LANES), jnp.bfloat16),
            pltpu.VMEM((2, chunks, 4, 48, LANES), jnp.bfloat16),
        ],
        compiler_params=pltpu.CompilerParams(collective_id=0, has_side_effects=True),
        name="dirac_twice",
    )(source_rows.reshape(6, rhs, 8, LANES), gauge_rows)
    out = rows.reshape(2, 3, rhs, 2, 4, LANES).transpose(0, 4, 1, 2, 3, 5)
    return out.reshape(source.shape)


def solution(mesh):
    spec = P("ta", "gz", None, None, None, None, None)
    return jax.shard_map(body, mesh=mesh, in_specs=(spec, spec), out_specs=spec, check_vma=False)
```

```python
import functools

import jax
import jax.numpy as jnp
from jax import lax
from jax.experimental import pallas as pl
from jax.experimental.pallas import tpu as pltpu
from jax.sharding import PartitionSpec as P

NX = 16
HOPPING = 0.124
GAMMA_PERM = ((3, 2, 1, 0), (3, 2, 1, 0), (2, 3, 0, 1), (2, 3, 0, 1))
GAMMA_PHASE = (
    ((0, 1), (0, 1), (0, -1), (0, -1)),
    ((-1, 0), (1, 0), (1, 0), (-1, 0)),
    ((0, 1), (0, -1), (0, -1), (0, 1)),
    ((1, 0), (1, 0), (1, 0), (1, 0)),
)
LANES = 128
MESH = pl.DeviceIdType.MESH
COMPONENTS = [(ri, s, c) for ri in range(2) for s in range(4) for c in range(3)]

HALOS = ((3, 1), (3, -1), (2, 1), (2, -1))


def signed_sum(base, term, sign):
    return base + term if sign > 0 else base - term


def project_row(psi, direction, hop_sign, s):
    partner = GAMMA_PERM[direction][s]
    pr, pi = GAMMA_PHASE[direction][s]
    row = []
    for c in range(3):
        if pi == 0:
            re = signed_sum(psi(0, s, c), psi(0, partner, c), -hop_sign * pr)
            im = signed_sum(psi(1, s, c), psi(1, partner, c), -hop_sign * pr)
        else:
            re = signed_sum(psi(0, s, c), psi(1, partner, c), hop_sign * pi)
            im = signed_sum(psi(1, s, c), psi(0, partner, c), -hop_sign * pi)
        row.append((re, im))
    return row


def color_product(link, row):
    out = []
    for r in range(3):
        re = im = None
        for c in range(3):
            lr, li = link(0, r, c), link(1, r, c)
            hr, hi = row[c]
            tr = lr * hr - li * hi
            ti = lr * hi + li * hr
            re = tr if re is None else re + tr
            im = ti if im is None else im + ti
        out.append((re, im))
    return out


def add_rebuilt(total, row, direction, hop_sign, s):
    low = GAMMA_PERM[direction].index(s)
    pr, pi = GAMMA_PHASE[direction][low]
    for c in range(3):
        kr, ki = row[c]
        total[0, s, c] = total[0, s, c] + kr
        total[1, s, c] = total[1, s, c] + ki
        if pi == 0:
            total[0, low, c] = signed_sum(total[0, low, c], kr, -hop_sign * pr)
            total[1, low, c] = signed_sum(total[1, low, c], ki, -hop_sign * pr)
        else:
            total[0, low, c] = signed_sum(total[0, low, c], ki, hop_sign * pi)
            total[1, low, c] = signed_sum(total[1, low, c], kr, -hop_sign * pi)


def packed(pair):
    return jnp.concatenate(pair, 0).astype(jnp.bfloat16)


def widened(tile):
    wide = tile.astype(jnp.float32)
    return wide[:8], wide[8:]


def shift_sites(tile, direction, steps):
    lane = lax.broadcasted_iota(jnp.int32, (8, LANES), 1)
    if direction == 0:
        column = lane % NX
        if steps > 0:
            return jnp.where(
                column == NX - 1,
                pltpu.roll(tile, NX - 1, axis=1),
                pltpu.roll(tile, LANES - 1, axis=1),
            )
        return jnp.where(
            column == 0,
            pltpu.roll(tile, LANES - (NX - 1), axis=1),
            pltpu.roll(tile, 1, axis=1),
        )
    near = pltpu.roll(tile, LANES - NX if steps > 0 else NX, axis=1)
    first_half = lax.broadcasted_iota(jnp.int32, (8, LANES), 0) % 2 == 0
    other = jnp.where(first_half, pltpu.roll(near, 7, axis=0), pltpu.roll(near, 1, axis=0))
    return jnp.where(lane >= LANES - NX if steps > 0 else lane < NX, other, near)


def plane(ri, s, c):
    return (ri * 4 + s) * 3 + c


def link_slot(direction, hop_sign):
    return direction * 2 + (0 if hop_sign > 0 else 1)


def apply_twice(
    groups, source_hbm, gauge_hbm, out, source, gauge, wide, psi, acc, links, sent, got,
    send_sem, final_sem,
):
    chunks = 2 * groups
    ta, gz = lax.axis_index("ta"), lax.axis_index("gz")
    nt, nz = lax.axis_size("ta"), lax.axis_size("gz")
    above_t = (lax.rem(ta + 1, nt), gz)
    below_t = (lax.rem(ta + nt - 1, nt), gz)
    above_z = (ta, lax.rem(gz + 1, nz))
    below_z = (ta, lax.rem(gz + nz - 1, nz))
    targets = (below_t, above_t, below_z, above_z)

    def landed(ref, semaphore):
        return pltpu.make_async_remote_copy(
            src_ref=ref, dst_ref=ref, send_sem=send_sem.at[0], recv_sem=semaphore,
            device_id=above_t, device_id_type=MESH,
        )

    def load_link(direction, hop_sign):
        slot = link_slot(direction, hop_sign)
        return lambda ri, r, c: links[slot, ri * 9 + r * 3 + c]

    def add_halo(total, step, slot, q, s, halo):
        direction, hop_sign = HALOS[halo]
        row = [widened(got[step, q, slot, 16 * c : 16 * c + 16]) for c in range(3)]
        if hop_sign > 0:
            row = color_product(load_link(direction, 1), row)
        add_rebuilt(total, row, direction, hop_sign, s)

    def rows_of(ri, s, c, g):
        return pl.ds(((ri * 3 + c) * groups + g) * 32 + s, 8, stride=4)

    def load_psi(step, g):
        return lambda ri, s, c: psi[step, g, plane(ri, s, c)]

    def plane_hops(step):
        def body(g, carry):
            at = load_psi(step, g)
            total = {key: at(*key) for key in COMPONENTS}
            for direction in (0, 1):
                for hop_sign in (1, -1):
                    for s in range(2):
                        row = [
                            tuple(shift_sites(v, direction, hop_sign) for v in pair)
                            for pair in project_row(at, direction, hop_sign, s)
                        ]
                        row = color_product(load_link(direction, hop_sign), row)
                        add_rebuilt(total, row, direction, hop_sign, s)
            for key, tile in total.items():
                acc[g, plane(*key)] = tile
            return carry

        lax.fori_loop(0, groups, body, 0)

    def first_application(load_sem, stage_sem, ready):
        def source_group(g):
            piece = pl.ds(4 * g, 4)
            return pltpu.make_async_copy(
                source_hbm.at[:, piece], source.at[:, piece], load_sem.at[g]
            )

        far_gauge = pltpu.make_async_copy(
            gauge_hbm.at[pl.ds(18, 18)], gauge.at[pl.ds(18, 18)], load_sem.at[groups]
        )
        near_gauge = pltpu.make_async_copy(
            gauge_hbm.at[pl.ds(0, 18)], gauge.at[pl.ds(0, 18)], load_sem.at[groups + 1]
        )
        for g in range(groups):
            source_group(g).start()
            if g == 0:
                far_gauge.start()
        near_gauge.start()

        barrier = pltpu.get_barrier_semaphore()

        def signal_when(condition, semaphore, target):
            @pl.when(condition)
            def _():
                pl.semaphore_signal(semaphore, inc=1, device_id=target, device_id_type=MESH)

        def wait_for(semaphore, *conditions):
            count = sum(c.astype(jnp.int32) for c in conditions)

            @pl.when(count > 0)
            def _():
                pl.semaphore_wait(semaphore, count)

        first_t, last_t, first_z, last_z = ta == 0, ta == nt - 1, gz == 0, gz == nz - 1
        stands_back = (lax.rem(ta, 2) == 1) & (ta > 1) & ~last_t
        met_below_t = (ta > 0) & (ta != nt // 2) & ~last_t
        met_above_t = last_t | (ta == nt // 2 - 1) | (ta == nt - 2)
        met_below_z, met_above_z = ~first_z, last_z
        signal_when(~met_above_t, barrier, above_t)
        signal_when(~met_below_t, barrier, below_t)
        signal_when(~met_above_z, barrier, above_z)
        signal_when(~met_below_z, barrier, below_z)
        wait_for(barrier, met_below_t, met_above_t, met_below_z, met_above_z)
        signal_when(met_above_z, ready.at[2], above_z)
        signal_when(met_below_z, ready.at[1], below_z)
        signal_when(met_below_t, ready.at[0], below_t)
        signal_when(met_above_t, ready.at[0], above_t)

        upper = (2 * gz) // nz

        def is_late(halo):
            there = (2 * lax.rem(gz + (nz - 1 if halo == 2 else 1), nz)) // nz
            return there if halo == 2 else 1 - there

        def start_halo(step, halo, q):
            if step == 1:
                slot, semaphore = halo, final_sem.at[jnp.maximum(q - (chunks - 3), 0)]
            elif halo < 2:
                slot, semaphore = halo, stage_sem.at[0, q]
            else:
                late = is_late(halo)
                slot, semaphore = 2 + late, stage_sem.at[late, q]
            pltpu.make_async_remote_copy(
                src_ref=sent.at[step, halo, q],
                dst_ref=got.at[step, q, slot],
                send_sem=send_sem.at[0],
                recv_sem=semaphore,
                device_id=targets[halo],
                device_id_type=MESH,
            ).start()

        def start_all(*halos, step=0):
            def one(q, carry):
                for condition, halo in halos:
                    @pl.when(condition)
                    def _():
                        start_halo(step, halo, q)
                return carry

            lax.fori_loop(0, chunks, one, 0)

        def put_halo(step, halo, q, s, at):
            direction, hop_sign = HALOS[halo]
            row = project_row(at, direction, hop_sign, s)
            if hop_sign < 0:
                row = color_product(load_link(direction, -1), row)
            for c in range(3):
                sent[step, halo, q, 16 * c : 16 * c + 16] = packed(row[c])

        first_half = lax.broadcasted_iota(jnp.int32, (8, LANES), 0) % 2 == 0

        def spread(rows, ri, scale):
            return scale * jnp.where(
                first_half,
                jnp.broadcast_to(rows[ri : ri + 1], (8, LANES)),
                jnp.broadcast_to(rows[2 + ri : 3 + ri], (8, LANES)),
            )

        def put_links(*directions):
            for direction in directions:
                scale = jnp.float32(-HOPPING)
                if direction == 3:
                    scale = jnp.where(last_t, HOPPING, -HOPPING).astype(jnp.float32)
                for r in range(3):
                    for c in range(3):
                        rows = gauge[direction * 9 + r * 3 + c].astype(jnp.float32)
                        for ri in range(2):
                            tile = spread(rows, ri, scale)
                            links[link_slot(direction, 1), ri * 9 + r * 3 + c] = tile
                            if direction < 2:
                                tile = shift_sites(tile, direction, -1)
                            links[link_slot(direction, -1), ri * 9 + c * 3 + r] = tile if ri == 0 else -tile

        def start_when(condition, halo, g):
            @pl.when(condition)
            def _():
                for s in range(2):
                    start_halo(0, halo, 2 * g + s)

        for g in range(groups):
            source_group(g).wait()
            for block in range(6):
                for p in range(4):
                    at = (block * groups + g) * 4 + p
                    wide[8 * at : 8 * at + 8] = source[block, 4 * g + p].astype(jnp.float32)
            tiles = {(ri, s, c): wide[rows_of(ri, s, c, g)] for ri, s, c in COMPONENTS}
            if g == 0:
                far_gauge.wait()
                put_links(3, 2)
            for halo in range(4):
                for s in range(2):
                    put_halo(0, halo, 2 * g + s, s, lambda *k: tiles[k])
            for k, tile in tiles.items():
                psi[0, g, plane(*k)] = tile
            start_when(met_below_t, 0, g)
            start_when(met_above_t, 1, g)
            start_when(last_z & ~stands_back, 3, g)
            start_when(met_below_z & ~last_z, 2, g)
        start_all((last_z, 2))
        wait_for(ready.at[1], ~met_above_z)
        start_all((~met_above_z, 3))
        wait_for(ready.at[0], ~met_above_t, ~met_below_t)
        start_all((~met_above_t, 1), (~met_below_t, 0))
        start_all((last_z & stands_back, 3))

        near_gauge.wait()
        put_links(0, 1)

        plane_hops(0)
        wait_for(ready.at[2], first_z)
        start_all((first_z, 2))

        held = last_z & (ta == 1)

        def stages(near, far):
            def early(g, carry):
                for s in range(2):
                    q = 2 * g + s
                    total = {k: acc[g, plane(*k)] for k in COMPONENTS if k[1] in (s, s + 2)}
                    landed(got.at[0, q, pl.ds(0, 3)], stage_sem.at[0, q]).wait_recv()
                    add_halo(total, 0, 0, q, s, 0)
                    add_halo(total, 0, 1, q, s, 1)
                    add_halo(total, 0, 2, q, s, near)
                    put_halo(1, near, q, s, lambda *k: total[k])
                    if near == 3:
                        @pl.when(~held)
                        def _():
                            start_halo(1, near, q)
                    else:
                        start_halo(1, near, q)
                    for k, tile in total.items():
                        acc[g, plane(*k)] = tile
                return carry

            def late(g, carry):
                for s in range(2):
                    q = 2 * g + s
                    total = {k: acc[g, plane(*k)] for k in COMPONENTS if k[1] in (s, s + 2)}
                    landed(got.at[0, q, 3], stage_sem.at[1, q]).wait_recv()
                    add_halo(total, 0, 3, q, s, far)
                    for s2 in (s, s + 2):
                        for c in range(3):
                            total[0, s2, c], total[1, s2, c] = widened(
                                packed([total[0, s2, c], total[1, s2, c]])
                            )
                    for halo in (0, 1, far):
                        put_halo(1, halo, q, s, lambda *k: total[k])
                    start_halo(1, 0, q)
                    start_halo(1, 1, q)
                    if far == 2:
                        @pl.when(~held)
                        def _():
                            start_halo(1, far, q)
                    else:
                        start_halo(1, far, q)
                    for k, tile in total.items():
                        psi[1, g, plane(*k)] = tile
                return carry

            lax.fori_loop(0, groups, early, 0)
            if near == 3:
                start_all((held, 3), step=1)
            lax.fori_loop(0, groups, late, 0)

        @pl.when(upper == 0)
        def _():
            stages(2, 3)

        @pl.when(upper == 1)
        def _():
            stages(3, 2)

        plane_hops(1)
        start_all((held, 2), step=1)

    pl.run_scoped(
        first_application,
        pltpu.SemaphoreType.DMA((groups + 2,)),
        pltpu.SemaphoreType.DMA((2, chunks)),
        pltpu.SemaphoreType.REGULAR((3,)),
    )

    for g in range(groups):
        for s in range(2):
            q = 2 * g + s
            total = {k: acc[g, plane(*k)] for k in COMPONENTS if k[1] in (s, s + 2)}
            if q == 0:
                landed(got.at[1, pl.ds(0, chunks - 2)], final_sem.at[0]).wait_recv()
            elif q > chunks - 3:
                landed(got.at[1, q], final_sem.at[q - (chunks - 3)]).wait_recv()
            for halo in range(4):
                add_halo(total, 1, halo, q, s, halo)
            for (ri, s2, c), tile in total.items():
                wide[rows_of(ri, s2, c, g)] = tile
        for block in range(6):
            for p in range(4):
                at = (block * groups + g) * 4 + p
                out[at] = wide[pl.ds(8 * at, 8)].astype(jnp.bfloat16)
    landed(sent, final_sem.at[0]).wait_send()


def kernel(groups, *refs):
    pl.run_scoped(
        functools.partial(apply_twice, groups, *refs),
        pltpu.SemaphoreType.DMA((1,)),
        pltpu.SemaphoreType.DMA((3,)),
    )


def body(source, gauge_field):
    rhs = source.shape[5]
    groups = rhs // 4
    chunks = 2 * groups
    source_rows = source.reshape(2, 4, 3, rhs, 2, LANES).transpose(0, 2, 3, 4, 1, 5)
    source_rows = source_rows.reshape(6 * rhs, 8, LANES)
    gauge_rows = gauge_field.reshape(4, 2, 3, 3, 2, LANES).transpose(0, 2, 3, 4, 1, 5)
    gauge_rows = gauge_rows.reshape(36, 4, LANES)
    rows = pl.pallas_call(
        functools.partial(kernel, groups),
        out_shape=pltpu.VMEM(source_rows.shape, source.dtype),
        in_specs=[pl.BlockSpec(memory_space=pltpu.HBM)] * 2,
        out_specs=pl.BlockSpec(memory_space=pltpu.VMEM),
        scratch_shapes=[
            pltpu.VMEM((6, rhs, 8, LANES), jnp.bfloat16),
            pltpu.VMEM(gauge_rows.shape, jnp.bfloat16),
            pltpu.VMEM((48 * rhs, LANES), jnp.float32),
            pltpu.VMEM((2, groups, 24, 8, LANES), jnp.float32),
            pltpu.VMEM((groups, 24, 8, LANES), jnp.float32),
            pltpu.VMEM((8, 18, 8, LANES), jnp.float32),
            pltpu.VMEM((2, 4, chunks, 48, LANES), jnp.bfloat16),
            pltpu.VMEM((2, chunks, 4, 48, LANES), jnp.bfloat16),
        ],
        compiler_params=pltpu.CompilerParams(collective_id=0, has_side_effects=True),
        name="dirac_twice",
    )(source_rows.reshape(6, rhs, 8, LANES), gauge_rows)
    out = rows.reshape(2, 3, rhs, 2, 4, LANES).transpose(0, 4, 1, 2, 3, 5)
    return out.reshape(source.shape)


def solution(mesh):
    spec = P("ta", "gz", None, None, None, None, None)
    return jax.shard_map(body, mesh=mesh, in_specs=(spec, spec), out_specs=spec, check_vma=False)
```
